128 devices in a mesh: row: 8 (over x, core), col: 16 (over z, y).
Axes of the slice: x: 4, y: 4, z: 4, core: 2. Of those that a mesh axis runs over, the one named last changes fastest.
Arguments:
- covariates: float32 [16, 32768], P(None, ('row', 'col')), may hold values from -6 to 6
- lengthscale: float32 [16], replicated, may hold values from 1 to 3
- nugget: float32 [32768], P(('row', 'col')), may hold values from 0.5 to 2
- patch_values: bfloat16 [32768, 16, 128], P(('row', 'col')), may hold values from -6 to 6
- patch_weights: bfloat16 [32768, 8, 128], P(('row', 'col')), may hold values from 0 to 0.1796875
- block_index: int32 [32768, 8], P(('row', 'col')), may hold values from 0 to 255
- slot_count: int32 [32768], P(('row', 'col')), may hold values from 1 to 8
- owner: int32 [32768, 1], P(('row', 'col')), may hold values from 0 to 127; in each aligned block of 256 rows (0 to 255, 256 to 511, ...) at most 4 rows name the same one
Outputs:
- solution: float32 [16, 32768], P(None, ('row', 'col'))
- residual: float32 [16, 32768], P(None, ('row', 'col'))
The draws below stay inside these ranges and needn't reach their ends.
Inputs may be any that keep to these rules, and one draw needn't show every extreme that they name: Among the 256 patches held by one device, no owner is named more than 4 times.
All inputs are finite; a program needn't handle non-finite values.
Results may differ from the reference program's by a relative error of at most 0.00045.
Values may be sent and summed in bfloat16 or wider, within the bound.
No kernel may reach another device: no remote copies, remote signals or barrier semaphores. Data moves between devices by JAX's collectives and lax.ppermute only.
A program may use at most 64 MiB of HBM per device.

```python
import math
import jax
import jax.numpy as jnp
import numpy as np
from jax import lax

FEATS = 16
MEMBERS = 16
CELLS = 128
SLOTS = 8
ST_DEV = 256
PATCH_DEV = 256
ITERS = 2
STATIONS = 32768
PATCHES = 32768
CAP = 4
DEVICES = 128


def touch_ends(array, stream_key, smallest, high):
    place = [jax.random.randint(jax.random.fold_in(stream_key, axis), (), 0, length) for axis, length in enumerate(array.shape)]
    widest = array.shape.index(max(array.shape))
    beside = place[:widest] + [(place[widest] + 1) % array.shape[widest]] + place[widest + 1:]
    return array.at[tuple(place)].set(smallest).at[tuple(beside)].set(high)


def steps_of(key, extent, shards, low, high):
    gain = 1.0
    for dim, parts in shards:
        steps = jax.random.uniform(jax.random.fold_in(jax.random.fold_in(key, 6), dim), (parts,), jnp.float32, low / len(shards), high / len(shards))
        gain = gain * jnp.repeat(jnp.exp(steps), extent[dim] // parts).reshape((-1,) + (1,) * (len(extent) - 1 - dim))
    return gain


def assign_block(key, own, number, rows, count, top, bound, skew):
    ranking = jax.random.permutation(key, count)
    crowded, common = portions_of(count, rows * top, bound, skew, True), portions_of(count, rows * top, bound, skew, False)
    places = jnp.arange(count)

    def named(lengths, turn):
        used = int((lengths > 0).sum())
        fixed = max(1, used // 4)
        passed = fixed + (places - fixed + turn * (used - fixed)) % max(1, count - fixed)
        return jnp.zeros((count,), jnp.int32).at[ranking[jnp.where(places < fixed, places, passed)]].set(jnp.asarray(lengths, jnp.int32))

    lengths = jnp.where(number % 4 == 0, named(crowded, number // 4), named(common, number - number // 4 - 1))
    mixed = jax.random.permutation(jax.random.fold_in(own, 3), count)
    giver, receiver = mixed[0:count // 2 * 2:2], mixed[1:count // 2 * 2:2]
    room = jnp.minimum(lengths[giver] - 1, bound - lengths[receiver]) // 2
    room = jnp.where((giver == ranking[0]) | (receiver == ranking[0]) | (lengths[receiver] == 0), 0, jnp.maximum(room, 0))
    passed = jax.random.randint(jax.random.fold_in(own, 4), (count // 2,), 0, 1 << 20) % (room + 1)
    lengths = lengths.at[giver].add(-passed).at[receiver].add(passed)
    labels = jnp.searchsorted(jnp.cumsum(lengths), jnp.arange(rows * top), side="right").astype(jnp.int32)
    grid = labels.reshape(top, rows).T
    grid = grid[jax.random.permutation(jax.random.fold_in(own, 1), rows)]
    turn = jax.random.randint(jax.random.fold_in(own, 2), (rows, 1), 0, top)
    return jnp.take_along_axis(grid, (jnp.arange(top)[None, :] + turn) % top, axis=1)


def portions_of(count, total, limit, skew, full):
    portions = [(1 << 20) // math.isqrt(standing ** skew) + 1 for standing in range(1, count + 1)]
    largest = limit if full else min(limit, max(-(-total // count), total * portions[0] // sum(portions)))
    least = 1 if total - largest >= count - 1 else 0
    given, surplus = [largest] + [least] * (count - 1), total - largest - least * (count - 1)
    while surplus > 0:
        movable = [i for i in range(1, count) if given[i] < largest] or [i for i in range(1, count) if given[i] < limit]
        whole, left = sum([portions[i] for i in movable]), surplus
        for i in movable:
            more = min(limit - given[i], max(1, left * portions[i] // whole), surplus)
            given[i] = given[i] + more
            surplus = surplus - more
    return np.array(given)


def gaussian(stream_key, extent, deviation, limit, pieces=(), held_as=jnp.bfloat16):
    drawn = deviation * jax.random.normal(stream_key, extent, jnp.float32)
    if pieces:
        drawn = drawn * steps_of(stream_key, extent, pieces, -0.22, 0.18)
    return jnp.clip(drawn, -limit, limit).astype(held_as)


def setup_inputs(seed: int = 0) -> dict:
    seeds = jax.random.split(jax.random.key(seed), 9)
    covariates = gaussian(seeds[0], (FEATS, STATIONS), 1.0, 6.0, ((1, 128),), jnp.float32)
    lengthscale = jnp.clip(jnp.exp(jax.random.uniform(seeds[1], (FEATS,), jnp.float32, math.log(1.0), math.log(3.0))), 1.0, 3.0)
    nugget = jnp.clip(jnp.exp(math.log(2.0) - 1.3862944 * jax.random.uniform(seeds[2], (STATIONS,), jnp.float32) ** steps_of(seeds[2], (STATIONS,), ((0, 128),), -0.2, 0.2)), 0.5, 2.0)
    patch_values = gaussian(seeds[3], (PATCHES, MEMBERS, CELLS), 1.0, 6.0, ((0, 128),))
    patch_weights = jnp.clip(0.1796875 * jax.random.uniform(seeds[4], (PATCHES, SLOTS, CELLS), jnp.float32) ** steps_of(seeds[4], (PATCHES, SLOTS, CELLS), ((0, 128),), -0.2, 0.2), 0.0, 0.1796875).astype(jnp.bfloat16)
    block_index = touch_ends(jax.random.randint(seeds[5], (PATCHES, SLOTS), 0, ST_DEV), jax.random.fold_in(seeds[5], 1), 0, ST_DEV - 1).astype(jnp.int32)
    slot_count = touch_ends(jax.random.randint(seeds[6], (PATCHES,), 1, SLOTS + 1), jax.random.fold_in(seeds[6], 1), 1, SLOTS).astype(jnp.int32)
    owner_keys = jax.random.split(jax.random.fold_in(seeds[7], 1), PATCHES // PATCH_DEV)
    owner_turns = jax.random.permutation(jax.random.fold_in(seeds[7], 3), PATCHES // PATCH_DEV)
    owner = jax.vmap(lambda own, number: assign_block(jax.random.fold_in(seeds[7], 2), own, number, PATCH_DEV, DEVICES, 1, CAP, 2))(owner_keys, owner_turns).reshape((PATCHES, 1))
    return dict(covariates=covariates, lengthscale=lengthscale, nugget=nugget, patch_values=patch_values, patch_weights=patch_weights, block_index=block_index, slot_count=slot_count, owner=owner)


ROOT_FIVE = 5.0 ** 0.5
HIGH = lax.Precision.HIGHEST

def matern(left, right):
    cross = lax.dot_general(left, right, (((0,), (0,)), ((), ())), precision=HIGH, preferred_element_type=jnp.float32)
    squared = lax.optimization_barrier(jnp.sum(left * left, axis=0))[:, None] + lax.optimization_barrier(jnp.sum(right * right, axis=0))[None, :] - 2.0 * cross
    scaled = ROOT_FIVE * jnp.sqrt(jnp.maximum(squared, 0.0))
    return (1.0 + scaled + scaled * scaled / 3.0) * jnp.exp(-scaled)

def apply_operator(direction, scaled_cov, nugget):
    width = math.gcd(STATIONS, 1024)
    count = STATIONS // width
    column_sets = jnp.transpose(scaled_cov.reshape(scaled_cov.shape[0], count, width), (1, 0, 2))

    def one_block(block_cov):
        return jnp.dot(direction, matern(scaled_cov, block_cov), precision=HIGH, preferred_element_type=jnp.float32)
    images = lax.map(one_block, column_sets)
    image = jnp.transpose(images, (1, 0, 2)).reshape(direction.shape[0], STATIONS)
    return image + nugget[None, :] * direction

def reference(covariates, lengthscale, nugget, patch_values, patch_weights, block_index, slot_count, owner):
    terms = jnp.einsum('psc,pmc->pms', patch_weights.astype(jnp.float32), patch_values.astype(jnp.float32))
    live = (jnp.arange(SLOTS, dtype=jnp.int32)[None, :] < slot_count[:, None]).astype(jnp.float32)
    terms = terms * live[:, None, :]
    station = (owner[:, 0][:, None] * ST_DEV + block_index).astype(jnp.int32)
    flat = jnp.transpose(terms, (0, 2, 1)).reshape(-1, MEMBERS)
    rhs = jax.ops.segment_sum(flat, station.reshape(-1), num_segments=STATIONS).T
    scaled_cov = covariates / lengthscale[:, None]
    solution = jnp.zeros_like(rhs)
    residual = rhs
    direction = rhs
    norm_now = lax.optimization_barrier(jnp.sum(residual * residual, axis=1))
    for step in range(ITERS):
        image = apply_operator(direction, scaled_cov, nugget)
        alpha = norm_now / lax.optimization_barrier(jnp.sum(direction * image, axis=1))
        solution = solution + alpha[:, None] * direction
        residual = residual - alpha[:, None] * image
        norm_next = lax.optimization_barrier(jnp.sum(residual * residual, axis=1))
        direction = residual + (norm_next / norm_now)[:, None] * direction
        norm_now = norm_next
    return (solution, residual)
```

```python
import math

import jax
import jax.numpy as jnp
from jax import lax
from jax.experimental import pallas as pl
from jax.experimental.pallas import tpu as pltpu
from jax.sharding import Mesh
from jax.sharding import PartitionSpec as P

ALL = ("row_0", "row_1", "col_0", "col_1")
COL = ("col_0", "col_1")
ROW = ("row_0", "row_1")

HIGH = lax.Precision.HIGHEST
LN2 = math.log(2.0)
SCALE = math.sqrt(5.0) / LN2
FACTOR = LN2 * LN2 / 3.0
LINEAR = 3.0 / LN2
CONST = 3.0 / (LN2 * LN2)
TINY = 1e-30
VMEM = pltpu.MemorySpace.VMEM
MIB = 1 << 20


def spread(shard, axes):
    copies = jnp.broadcast_to(shard[None], (lax.axis_size(axes),) + shard.shape)
    return lax.all_to_all(copies, axes, split_axis=0, concat_axis=0, tiled=True)


def halves(x):
    high = x.astype(jnp.bfloat16).astype(jnp.float32)
    return high, x - high


def thirds(x):
    high, rest = halves(x)
    middle, low = halves(rest)
    return high, middle, low


def features(z, left):
    high, middle, low = thirds(z)
    norm = jnp.sum(z * z, axis=0, keepdims=True)
    n_high, n_middle, n_low = thirds(norm)
    row = lax.broadcasted_iota(jnp.int32, z.shape, 0)
    base = 0 if left else 3
    rest = jnp.zeros_like(z)
    for at, part in ((base, n_high), (base + 1, n_middle), (base + 2, n_low)):
        rest = jnp.where(row == at, jnp.broadcast_to(part, z.shape), rest)
    rest = jnp.where((row >= 3 - base) & (row < 6 - base), 1.0, rest)
    if left:
        parts = [high, high, high, middle, middle, low]
    else:
        parts = [-2.0 * part for part in (high, middle, low, high, middle, high)]
    return jnp.concatenate(parts + [rest, jnp.zeros_like(z)], axis=0)


def kernel_body(zj_ref, zi_ref, high_ref, low_ref, fj_ref, fi_ref):
    width = zj_ref.shape[2]
    for r in range(zj_ref.shape[0]):
        block = features(zj_ref[r] * SCALE, True)
        fj_ref[r * width : (r + 1) * width, :] = jnp.transpose(block).astype(jnp.bfloat16)
    for c in range(zi_ref.shape[0]):
        block = features(zi_ref[c] * SCALE, False)
        fi_ref[:, c * width : (c + 1) * width] = block.astype(jnp.bfloat16)
    tall, wide = 256, 1024
    across = fi_ref.shape[1] // wide

    @pl.loop(0, (fj_ref.shape[0] // tall) * across)
    def _(step):
        rows = pl.ds(pl.multiple_of((step // across) * tall, tall), tall)
        columns = pl.ds(pl.multiple_of((step % across) * wide, wide), wide)
        squared = jnp.dot(
            fj_ref[rows, :], fi_ref[:, columns], preferred_element_type=jnp.float32
        )
        squared = jnp.maximum(squared, TINY)
        root = squared * lax.rsqrt(squared)
        value = (squared + (LINEAR * root + CONST)) * jnp.exp2(-root)
        high = value.astype(jnp.bfloat16)
        high_ref[rows, columns] = high
        low_ref[rows, columns] = (value - high.astype(jnp.float32)).astype(jnp.bfloat16)


def build_kernel(zj, zi):
    rows, columns = zj.shape[0] * zj.shape[2], zi.shape[0] * zi.shape[2]
    return pl.pallas_call(
        kernel_body,
        out_shape=[pltpu.VMEM((rows, columns), jnp.bfloat16)] * 2,
        in_specs=[pl.BlockSpec(memory_space=VMEM)] * 2,
        out_specs=[pl.BlockSpec(memory_space=VMEM)] * 2,
        scratch_shapes=[
            pltpu.VMEM((rows, 128), jnp.bfloat16),
            pltpu.VMEM((128, columns), jnp.bfloat16),
        ],
        compiler_params=pltpu.CompilerParams(vmem_limit_bytes=12 * MIB),
        cost_estimate=pl.CostEstimate(
            flops=40 * rows * columns, bytes_accessed=4 * rows * columns, transcendentals=0
        ),
        name="matern",
    )(zj, zi)


def product_body(v_ref, high_ref, low_ref, out_ref, vv_ref):
    count, members, width = v_ref.shape
    for r in range(count):
        high, low = halves(v_ref[r])
        columns = slice(r * width, (r + 1) * width)
        vv_ref[:members, columns] = high.astype(jnp.bfloat16)
        vv_ref[members:, columns] = low.astype(jnp.bfloat16)
    wide = 2 * width

    @pl.loop(0, high_ref.shape[1] // wide)
    def _(step):
        columns = pl.ds(pl.multiple_of(step * wide, wide), wide)
        vv = vv_ref[...]
        both = jnp.dot(vv, high_ref[:, columns], preferred_element_type=jnp.float32)
        both += jnp.dot(vv, low_ref[:, columns], preferred_element_type=jnp.float32)
        total = FACTOR * (both[:members] + both[members:])
        for t in range(2):
            out_ref[step * 2 + t] = total[:, t * width : (t + 1) * width]


def kernel_product(v, high, low):
    count, members, width = v.shape
    rows, columns = high.shape
    return pl.pallas_call(
        product_body,
        out_shape=jax.ShapeDtypeStruct((columns // width, members, width), jnp.float32),
        in_specs=[pl.BlockSpec(memory_space=VMEM)] * 3,
        out_specs=pl.BlockSpec(memory_space=VMEM),
        scratch_shapes=[pltpu.VMEM((2 * members, rows), jnp.bfloat16)],
        compiler_params=pltpu.CompilerParams(vmem_limit_bytes=12 * MIB),
        cost_estimate=pl.CostEstimate(
            flops=128 * rows * columns, bytes_accessed=4 * rows * columns, transcendentals=0
        ),
        name="product",
    )(v, high, low)


def local(
    covariates, lengthscale, nugget, patch_values, patch_weights, block_index, slot_count, owner
):
    devices = lax.axis_size(ALL)
    held, members, cells = patch_values.shape
    slots = patch_weights.shape[1]
    stations = nugget.shape[0]
    capacity = max(2, 2 * held // devices)

    terms = jnp.einsum(
        "psc,pmc->psm", patch_weights, patch_values, preferred_element_type=jnp.float32
    )
    live = (jnp.arange(slots)[None, :] < slot_count[:, None]).astype(jnp.float32)
    terms = (terms * live[:, :, None]).reshape(held, slots * members)
    target = owner[:, 0]
    earlier = jnp.arange(held)[None, :] < jnp.arange(held)[:, None]
    rank = jnp.sum(((target[:, None] == target[None, :]) & earlier).astype(jnp.int32), axis=1)
    position = rank * devices + target
    table = (position[None, :] == jnp.arange(devices * capacity)[:, None]).astype(jnp.float32)
    payload = jnp.concatenate([terms, block_index.astype(jnp.float32)], axis=1)
    placed = jnp.dot(table, payload, precision=HIGH, preferred_element_type=jnp.float32)
    placed = placed.reshape(capacity, devices, payload.shape[1])
    message = jnp.concatenate(
        [placed[k, :, : slots * members] for k in range(capacity)]
        + [placed[k, :, slots * members :] for k in range(capacity)],
        axis=1,
    )
    message = lax.all_to_all(message, ALL, split_axis=0, concat_axis=0, tiled=True)

    scaled_cov = covariates / lengthscale[:, None]
    high, low = build_kernel(spread(scaled_cov, ROW), spread(scaled_cov, COL))

    entries = capacity * slots
    flat = message[:, : entries * members].reshape(devices, entries, members)
    index = message[:, entries * members :].astype(jnp.int32)
    onehot = (index.reshape(-1)[:, None] == jnp.arange(stations)[None, :]).astype(jnp.float32)
    rhs = lax.dot_general(
        flat.reshape(-1, members),
        onehot,
        (((0,), (0,)), ((), ())),
        precision=HIGH,
        preferred_element_type=jnp.float32,
    )

    def operate(v):
        partial_value = kernel_product(spread(v, ROW), high, low)
        shares = lax.all_to_all(partial_value, COL, split_axis=0, concat_axis=0, tiled=True)
        return jnp.sum(shares, axis=0) + nugget[None, :] * v

    first = operate(rhs)
    second = operate(first)

    def dot(a, b):
        return jnp.sum(a * b, axis=1)

    norm, energy = dot(rhs, rhs), dot(rhs, first)
    guess = jnp.where(energy > 0.5 * norm, norm / jnp.maximum(energy, TINY), 0.0)
    resid = rhs - guess[:, None] * first
    along = first - guess[:, None] * second
    sums = jnp.stack(
        [
            norm,
            energy,
            guess,
            dot(resid, resid),
            dot(resid, first),
            dot(first, first),
            dot(resid, along),
            dot(resid, second) + dot(first, along),
            dot(first, second),
        ]
    ).reshape(1, -1)
    sums = jnp.pad(sums, ((0, 0), (0, -sums.shape[1] % 128)))
    sums = spread(sums, ALL)[:, 0, : 9 * members].reshape(devices, 9, members)
    norm0 = jnp.sum(sums[:, 0], axis=0)
    alpha0 = norm0 / jnp.sum(sums[:, 1], axis=0)
    shift = alpha0[None, :] - sums[:, 2]
    norm1 = jnp.sum(sums[:, 3] - shift * (2.0 * sums[:, 4] - shift * sums[:, 5]), axis=0)
    energy1 = jnp.sum(sums[:, 6] - shift * (sums[:, 7] - shift * sums[:, 8]), axis=0)
    ratio = norm1 / norm0
    alpha1 = norm1 / (energy1 - ratio * norm1 / alpha0)
    residual = rhs - alpha0[:, None] * first
    direction = residual + ratio[:, None] * rhs
    along = (first - alpha0[:, None] * second) + ratio[:, None] * first
    solved = alpha0[:, None] * rhs + alpha1[:, None] * direction
    return (solved, residual - alpha1[:, None] * along)


def solution(mesh):
    torus = Mesh(mesh.devices.reshape(4, 2, 4, 4), ALL)
    placed = (
        P(None, ALL),
        P(),
        P(ALL),
        P(ALL, None, None),
        P(ALL, None, None),
        P(ALL, None),
        P(ALL),
        P(ALL, None),
    )
    return jax.shard_map(
        local,
        mesh=torus,
        in_specs=placed,
        out_specs=(P(None, ALL), P(None, ALL)),
        check_vma=False,
    )
```

```python
import math

import jax
import jax.numpy as jnp
from jax import lax
from jax.experimental import pallas as pl
from jax.experimental.pallas import tpu as pltpu
from jax.sharding import Mesh
from jax.sharding import PartitionSpec as P

ALL = ("row_0", "row_1", "col_0", "col_1")
COL = ("col_0", "col_1")
ROW = ("row_0", "row_1")

HIGH = lax.Precision.HIGHEST
LN2 = math.log(2.0)
SCALE = math.sqrt(5.0) / LN2
FACTOR = LN2 * LN2 / 3.0
LINEAR = 3.0 / LN2
CONST = 3.0 / (LN2 * LN2)
TINY = 1e-30
VMEM = pltpu.MemorySpace.VMEM
MIB = 1 << 20


def spread(shard, axes):
    copies = jnp.broadcast_to(shard[None], (lax.axis_size(axes),) + shard.shape)
    return lax.all_to_all(copies, axes, split_axis=0, concat_axis=0, tiled=True)


def halves(x):
    high = x.astype(jnp.bfloat16).astype(jnp.float32)
    return high, x - high


def thirds(x):
    high, rest = halves(x)
    middle, low = halves(rest)
    return high, middle, low


def features(z, left):
    high, middle, low = thirds(z)
    norm = jnp.sum(z * z, axis=0, keepdims=True)
    n_high, n_middle, n_low = thirds(norm)
    row = lax.broadcasted_iota(jnp.int32, z.shape, 0)
    base = 0 if left else 3
    rest = jnp.zeros_like(z)
    for at, part in ((base, n_high), (base + 1, n_middle), (base + 2, n_low)):
        rest = jnp.where(row == at, jnp.broadcast_to(part, z.shape), rest)
    rest = jnp.where((row >= 3 - base) & (row < 6 - base), 1.0, rest)
    if left:
        parts = [high, high, high, middle, middle, low]
    else:
        parts = [-2.0 * part for part in (high, middle, low, high, middle, high)]
    return jnp.concatenate(parts + [rest, jnp.zeros_like(z)], axis=0)


def kernel_body(zj_ref, zi_ref, high_ref, low_ref, fj_ref, fi_ref):
    width = zj_ref.shape[2]
    for r in range(zj_ref.shape[0]):
        block = features(zj_ref[r] * SCALE, True)
        fj_ref[r * width : (r + 1) * width, :] = jnp.transpose(block).astype(jnp.bfloat16)
    for c in range(zi_ref.shape[0]):
        block = features(zi_ref[c] * SCALE, False)
        fi_ref[:, c * width : (c + 1) * width] = block.astype(jnp.bfloat16)
    tall, wide = 256, 1024
    across = fi_ref.shape[1] // wide

    @pl.loop(0, (fj_ref.shape[0] // tall) * across)
    def _(step):
        rows = pl.ds(pl.multiple_of((step // across) * tall, tall), tall)
        columns = pl.ds(pl.multiple_of((step % across) * wide, wide), wide)
        squared = jnp.dot(
            fj_ref[rows, :], fi_ref[:, columns], preferred_element_type=jnp.float32
        )
        squared = jnp.maximum(squared, TINY)
        root = squared * lax.rsqrt(squared)
        value = (squared + (LINEAR * root + CONST)) * jnp.exp2(-root)
        high = value.astype(jnp.bfloat16)
        high_ref[rows, columns] = high
        low_ref[rows, columns] = (value - high.astype(jnp.float32)).astype(jnp.bfloat16)


def build_kernel(zj, zi):
    rows, columns = zj.shape[0] * zj.shape[2], zi.shape[0] * zi.shape[2]
    return pl.pallas_call(
        kernel_body,
        out_shape=[pltpu.VMEM((rows, columns), jnp.bfloat16)] * 2,
        in_specs=[pl.BlockSpec(memory_space=VMEM)] * 2,
        out_specs=[pl.BlockSpec(memory_space=VMEM)] * 2,
        scratch_shapes=[
            pltpu.VMEM((rows, 128), jnp.bfloat16),
            pltpu.VMEM((128, columns), jnp.bfloat16),
        ],
        compiler_params=pltpu.CompilerParams(vmem_limit_bytes=12 * MIB),
        cost_estimate=pl.CostEstimate(
            flops=40 * rows * columns, bytes_accessed=4 * rows * columns, transcendentals=0
        ),
        name="matern",
    )(zj, zi)


def product_body(v_ref, high_ref, low_ref, out_ref, vv_ref):
    count, members, width = v_ref.shape
    for r in range(count):
        high, low = halves(v_ref[r])
        columns = slice(r * width, (r + 1) * width)
        vv_ref[:members, columns] = high.astype(jnp.bfloat16)
        vv_ref[members:, columns] = low.astype(jnp.bfloat16)
    wide = 2 * width

    @pl.loop(0, high_ref.shape[1] // wide)
    def _(step):
        columns = pl.ds(pl.multiple_of(step * wide, wide), wide)
        vv = vv_ref[...]
        both = jnp.dot(vv, high_ref[:, columns], preferred_element_type=jnp.float32)
        both += jnp.dot(vv, low_ref[:, columns], preferred_element_type=jnp.float32)
        total = FACTOR * (both[:members] + both[members:])
        for t in range(2):
            out_ref[step * 2 + t] = total[:, t * width : (t + 1) * width]


def kernel_product(v, high, low):
    count, members, width = v.shape
    rows, columns = high.shape
    return pl.pallas_call(
        product_body,
        out_shape=jax.ShapeDtypeStruct((columns // width, members, width), jnp.float32),
        in_specs=[pl.BlockSpec(memory_space=VMEM)] * 3,
        out_specs=pl.BlockSpec(memory_space=VMEM),
        scratch_shapes=[pltpu.VMEM((2 * members, rows), jnp.bfloat16)],
        compiler_params=pltpu.CompilerParams(vmem_limit_bytes=12 * MIB),
        cost_estimate=pl.CostEstimate(
            flops=128 * rows * columns, bytes_accessed=4 * rows * columns, transcendentals=0
        ),
        name="product",
    )(v, high, low)


def total_body(shares_ref, v_ref, nugget_ref, out_ref, copies_ref):
    total = nugget_ref[...] * v_ref[...]
    for c in range(shares_ref.shape[0]):
        total += shares_ref[c]
    out_ref[...] = total
    for r in range(copies_ref.shape[0]):
        copies_ref[r] = total


def total_of(shares, v, nugget, copies):
    return pl.pallas_call(
        total_body,
        out_shape=[
            jax.ShapeDtypeStruct(v.shape, jnp.float32),
            jax.ShapeDtypeStruct((copies,) + v.shape, jnp.float32),
        ],
        in_specs=[pl.BlockSpec(memory_space=VMEM)] * 3,
        out_specs=[pl.BlockSpec(memory_space=VMEM)] * 2,
        compiler_params=pltpu.CompilerParams(vmem_limit_bytes=4 * MIB),
        name="total",
    )(shares, v, nugget)


def guess_of(norm, energy):
    usable = energy > 0.5 * norm
    return jnp.where(usable, norm / jnp.where(usable, energy, 1.0), 0.0)


def close_body(shares_ref, rhs_ref, first_ref, nugget_ref, second_ref, sums_ref):
    rhs, first = rhs_ref[...], first_ref[...]
    second = nugget_ref[...] * first
    for c in range(shares_ref.shape[0]):
        second += shares_ref[c]
    second_ref[...] = second

    def dot(a, b):
        return jnp.sum(a * b, axis=1, keepdims=True)

    norm, energy = dot(rhs, rhs), dot(rhs, first)
    guess = guess_of(norm, energy)
    resid = rhs - guess * first
    along = first - guess * second
    sums = [
        norm,
        energy,
        dot(resid, resid),
        dot(resid, first),
        dot(first, first),
        dot(resid, along),
        dot(resid, second) + dot(first, along),
        dot(first, second),
    ]
    members = rhs.shape[0]
    shape = (members, len(sums) * members)
    row = lax.broadcasted_iota(jnp.int32, shape, 0)
    lane = lax.broadcasted_iota(jnp.int32, shape, 1)
    spaced = jnp.zeros(shape, jnp.float32)
    for at, column in enumerate(sums):
        here = lane == row + at * members
        spaced += jnp.where(here, jnp.broadcast_to(column, shape), 0.0)
    sums_ref[...] = jnp.sum(spaced, axis=0, keepdims=True)


def close(shares, rhs, first, nugget):
    members = rhs.shape[0]
    return pl.pallas_call(
        close_body,
        out_shape=[
            jax.ShapeDtypeStruct(rhs.shape, jnp.float32),
            jax.ShapeDtypeStruct((1, 8 * members), jnp.float32),
        ],
        in_specs=[pl.BlockSpec(memory_space=VMEM)] * 4,
        out_specs=[pl.BlockSpec(memory_space=VMEM)] * 2,
        compiler_params=pltpu.CompilerParams(vmem_limit_bytes=4 * MIB),
        name="close",
    )(shares, rhs, first, nugget)


def finish_body(sums_ref, rhs_ref, first_ref, second_ref, solved_ref, residual_ref):
    rhs, first, second = rhs_ref[...], first_ref[...], second_ref[...]
    members = rhs.shape[0]
    norm, energy, rr, rf, ff, ra, rs, fs = (
        sums_ref[:, q * members : (q + 1) * members] for q in range(8)
    )

    def over(x):
        return jnp.sum(x, axis=0, keepdims=True)

    norm0 = over(norm)
    alpha0 = norm0 / over(energy)
    shift = alpha0 - guess_of(norm, energy)
    norm1 = over(rr - shift * (2.0 * rf - shift * ff))
    energy1 = over(ra - shift * (rs - shift * fs))
    ratio = norm1 / norm0
    alpha1 = norm1 / (energy1 - ratio * norm1 / alpha0)
    shape = (members, members)
    same = lax.broadcasted_iota(jnp.int32, shape, 0) == lax.broadcasted_iota(jnp.int32, shape, 1)

    def column(x):
        return jnp.sum(jnp.where(same, jnp.broadcast_to(x, shape), 0.0), axis=1, keepdims=True)

    alpha0, alpha1, ratio = column(alpha0), column(alpha1), column(ratio)
    residual = rhs - alpha0 * first
    direction = residual + ratio * rhs
    along = (first - alpha0 * second) + ratio * first
    solved_ref[...] = alpha0 * rhs + alpha1 * direction
    residual_ref[...] = residual - alpha1 * along


def finish(sums, rhs, first, second):
    return pl.pallas_call(
        finish_body,
        out_shape=[jax.ShapeDtypeStruct(rhs.shape, jnp.float32)] * 2,
        in_specs=[pl.BlockSpec(memory_space=VMEM)] * 4,
        out_specs=[pl.BlockSpec(memory_space=VMEM)] * 2,
        compiler_params=pltpu.CompilerParams(vmem_limit_bytes=4 * MIB),
        name="finish",
    )(sums, rhs, first, second)


def exchange(pieces, axes):
    return lax.all_to_all(pieces, axes, split_axis=0, concat_axis=0, tiled=True)


def local(
    covariates, lengthscale, nugget, patch_values, patch_weights, block_index, slot_count, owner
):
    devices = lax.axis_size(ALL)
    held, members, cells = patch_values.shape
    slots = patch_weights.shape[1]
    stations = nugget.shape[0]
    capacity = max(2, 2 * held // devices)

    scaled_cov = covariates / lengthscale[:, None]
    column_cov, row_cov = spread(scaled_cov, ROW), spread(scaled_cov, COL)

    terms = jnp.einsum(
        "psc,pmc->psm", patch_weights, patch_values, preferred_element_type=jnp.float32
    )
    live = (jnp.arange(slots)[None, :] < slot_count[:, None]).astype(jnp.float32)
    terms = (terms * live[:, :, None]).reshape(held, slots * members)
    target = owner[:, 0]
    earlier = jnp.arange(held)[None, :] < jnp.arange(held)[:, None]
    rank = jnp.sum(((target[:, None] == target[None, :]) & earlier).astype(jnp.int32), axis=1)
    position = rank * devices + target
    table = (position[None, :] == jnp.arange(devices * capacity)[:, None]).astype(jnp.float32)
    payload = jnp.concatenate([terms, block_index.astype(jnp.float32)], axis=1)
    placed = jnp.dot(table, payload, precision=HIGH, preferred_element_type=jnp.float32)
    placed = placed.reshape(capacity, devices, payload.shape[1])
    message = jnp.concatenate(
        [placed[k, :, : slots * members] for k in range(capacity)]
        + [placed[k, :, slots * members :] for k in range(capacity)],
        axis=1,
    )
    message = lax.all_to_all(message, ALL, split_axis=0, concat_axis=0, tiled=True)

    entries = capacity * slots
    flat = message[:, : entries * members].reshape(devices, entries, members)
    index = message[:, entries * members :].astype(jnp.int32)
    onehot = (index.reshape(-1)[:, None] == jnp.arange(stations)[None, :]).astype(jnp.float32)
    rhs = lax.dot_general(
        flat.reshape(-1, members),
        onehot,
        (((0,), (0,)), ((), ())),
        precision=HIGH,
        preferred_element_type=jnp.float32,
    )

    gathered = spread(rhs, ROW)
    gathered, column_cov, row_cov = lax.optimization_barrier((gathered, column_cov, row_cov))
    high, low = build_kernel(column_cov, row_cov)
    nugget = nugget[None, :]
    shares = exchange(kernel_product(gathered, high, low), COL)
    first, copies = total_of(shares, rhs, nugget, lax.axis_size(ROW))
    shares = exchange(kernel_product(exchange(copies, ROW), high, low), COL)
    second, sums = close(shares, rhs, first, nugget)
    copies = jnp.broadcast_to(sums[None], (devices,) + sums.shape)
    sums = exchange(copies, ALL).reshape(devices, sums.shape[1])
    return finish(sums, rhs, first, second)


def solution(mesh):
    torus = Mesh(mesh.devices.reshape(4, 2, 4, 4), ALL)
    placed = (
        P(None, ALL),
        P(),
        P(ALL),
        P(ALL, None, None),
        P(ALL, None, None),
        P(ALL, None),
        P(ALL),
        P(ALL, None),
    )
    return jax.shard_map(
        local,
        mesh=torus,
        in_specs=placed,
        out_specs=(P(None, ALL), P(None, ALL)),
        check_vma=False,
    )
```

```python
import functools
import math

import jax
import jax.numpy as jnp
from jax import lax
from jax.experimental import pallas as pl
from jax.experimental.pallas import tpu as pltpu
from jax.sharding import Mesh
from jax.sharding import PartitionSpec as P

ALL = ("row_0", "row_1", "col_0", "col_1")
COL = ("col_0", "col_1")
ROW = ("row_0", "row_1")

LN2 = math.log(2.0)
SCALE = math.sqrt(5.0) / LN2
FACTOR = LN2 * LN2 / 3.0
LINEAR = 3.0 / LN2
CONST = 3.0 / (LN2 * LN2)
TINY = 1e-30
TILE, TILES = 512, 4
VMEM = pltpu.MemorySpace.VMEM
MIB = 1 << 20


def spread(shard, axes):
    copies = jnp.broadcast_to(shard[None], (lax.axis_size(axes),) + shard.shape)
    return lax.all_to_all(copies, axes, split_axis=0, concat_axis=0, tiled=True)


def halves(x):
    high = x.astype(jnp.bfloat16).astype(jnp.float32)
    return high, x - high


def thirds(x):
    high, rest = halves(x)
    middle, low = halves(rest)
    return high, middle, low


def features(z, left):
    high, middle, low = thirds(z)
    norm = jnp.sum(z * z, axis=0, keepdims=True)
    n_high, n_middle, n_low = thirds(norm)
    row = lax.broadcasted_iota(jnp.int32, z.shape, 0)
    base = 0 if left else 3
    rest = jnp.zeros_like(z)
    for at, part in ((base, n_high), (base + 1, n_middle), (base + 2, n_low)):
        rest = jnp.where(row == at, jnp.broadcast_to(part, z.shape), rest)
    rest = jnp.where((row >= 3 - base) & (row < 6 - base), 1.0, rest)
    if left:
        parts = [high, high, high, middle, middle, low]
    else:
        parts = [-2.0 * part for part in (high, middle, low, high, middle, high)]
    return jnp.concatenate(parts + [rest, jnp.zeros_like(z)], axis=0)


def value_of(squared):
    squared = jnp.maximum(squared, TINY)
    root = squared * lax.rsqrt(squared)
    return (squared + (LINEAR * root + CONST)) * jnp.exp2(-root)


def split_vector(v_ref, first, vv_ref):
    width = v_ref.shape[2]
    members = vv_ref.shape[0] // 2
    for r in range(v_ref.shape[0]):
        high, low = halves(v_ref[r, first : first + members])
        columns = slice(r * width, (r + 1) * width)
        vv_ref[:members, columns] = high.astype(jnp.bfloat16)
        vv_ref[members:, columns] = low.astype(jnp.bfloat16)


def build_body(
    zv_ref, zi_ref, high_ref, low_ref, out_ref, fj_ref, fi_ref, vv_ref, acc_ref, ahead_ref
):
    feats, members, width = zi_ref.shape[1], vv_ref.shape[0] // 2, zi_ref.shape[2]
    for r in range(zv_ref.shape[0]):
        block = features(zv_ref[r, :feats] * SCALE, True)
        fj_ref[r * width : (r + 1) * width, :] = jnp.transpose(block.astype(jnp.bfloat16))
    for c in range(zi_ref.shape[0]):
        block = features(zi_ref[c] * SCALE, False)
        fi_ref[:, c * width : (c + 1) * width] = block.astype(jnp.bfloat16)
    split_vector(zv_ref, feats, vv_ref)
    acc_ref[...] = jnp.zeros_like(acc_ref)
    tall, wide, tiles = width, TILE, TILES
    across = fi_ref.shape[1] // (wide * tiles)
    steps = across * (fj_ref.shape[0] // tall)

    def place(step, tile):
        rows = pl.ds(pl.multiple_of((step // across) * tall, tall), tall)
        columns = ((step % across) * tiles + tile) * wide
        return rows, pl.ds(pl.multiple_of(columns, wide), wide)

    def squares(step, tile):
        rows, columns = place(step, tile)
        return jnp.dot(fj_ref[rows, :], fi_ref[:, columns], preferred_element_type=jnp.float32)

    ahead_ref[...] = squares(0, 0)

    @pl.loop(0, steps)
    def _(step):
        squared = ahead_ref[...]
        for tile in range(tiles):
            if tile + 1 < tiles:
                ahead = squares(step, tile + 1)
            else:
                ahead = squares(jnp.minimum(step + 1, steps - 1), 0)
            rows, columns = place(step, tile)
            value = value_of(squared)
            high = value.astype(jnp.bfloat16)
            low = (value - high.astype(jnp.float32)).astype(jnp.bfloat16)
            high_ref[rows, columns] = high
            low_ref[rows, columns] = low
            vv = vv_ref[:, rows]
            acc_ref[:, columns] += jnp.dot(
                vv, high, preferred_element_type=jnp.float32
            ) + jnp.dot(vv, low, preferred_element_type=jnp.float32)
            squared = ahead
        ahead_ref[...] = squared

    for c in range(out_ref.shape[0]):
        columns = slice(c * width, (c + 1) * width)
        out_ref[c] = FACTOR * (acc_ref[:members, columns] + acc_ref[members:, columns])


def build_and_product(zv, zi):
    feats, width = zi.shape[1], zi.shape[2]
    members = zv.shape[1] - feats
    rows, columns = zv.shape[0] * width, zi.shape[0] * width
    return pl.pallas_call(
        build_body,
        out_shape=[pltpu.VMEM((rows, columns), jnp.bfloat16)] * 2
        + [jax.ShapeDtypeStruct((zi.shape[0], members, width), jnp.float32)],
        in_specs=[pl.BlockSpec(memory_space=VMEM)] * 2,
        out_specs=[pl.BlockSpec(memory_space=VMEM)] * 3,
        scratch_shapes=[
            pltpu.VMEM((rows, 128), jnp.bfloat16),
            pltpu.VMEM((128, columns), jnp.bfloat16),
            pltpu.VMEM((2 * members, rows), jnp.bfloat16),
            pltpu.VMEM((2 * members, columns), jnp.float32),
            pltpu.VMEM((width, TILE), jnp.float32),
        ],
        compiler_params=pltpu.CompilerParams(vmem_limit_bytes=12 * MIB),
        cost_estimate=pl.CostEstimate(
            flops=40 * rows * columns, bytes_accessed=4 * rows * columns, transcendentals=0
        ),
        name="build",
    )(zv, zi)


def product_body(v_ref, high_ref, low_ref, out_ref, vv_ref):
    count, members, width = v_ref.shape
    split_vector(v_ref, 0, vv_ref)
    wide = 2 * width

    @pl.loop(0, high_ref.shape[1] // wide)
    def _(step):
        columns = pl.ds(pl.multiple_of(step * wide, wide), wide)
        vv = vv_ref[...]
        both = jnp.dot(vv, high_ref[:, columns], preferred_element_type=jnp.float32)
        both += jnp.dot(vv, low_ref[:, columns], preferred_element_type=jnp.float32)
        total = FACTOR * (both[:members] + both[members:])
        for t in range(2):
            out_ref[step * 2 + t] = total[:, t * width : (t + 1) * width]


def kernel_product(v, high, low):
    count, members, width = v.shape
    rows, columns = high.shape
    return pl.pallas_call(
        product_body,
        out_shape=jax.ShapeDtypeStruct((columns // width, members, width), jnp.float32),
        in_specs=[pl.BlockSpec(memory_space=VMEM)] * 3,
        out_specs=pl.BlockSpec(memory_space=VMEM),
        scratch_shapes=[pltpu.VMEM((2 * members, rows), jnp.bfloat16)],
        compiler_params=pltpu.CompilerParams(vmem_limit_bytes=12 * MIB),
        cost_estimate=pl.CostEstimate(
            flops=128 * rows * columns, bytes_accessed=4 * rows * columns, transcendentals=0
        ),
        name="product",
    )(v, high, low)


def to_column(row, size):
    shape = (size, row.shape[1])
    same = lax.broadcasted_iota(jnp.int32, shape, 0) == lax.broadcasted_iota(jnp.int32, shape, 1)
    return jnp.sum(jnp.where(same, jnp.broadcast_to(row, shape), 0.0), axis=1, keepdims=True)


def terms_body(capacity, values_ref, weights_ref, index_ref, count_ref, owner_ref, out_ref, t_ref):
    slots, held = index_ref.shape
    members = values_ref.shape[0] // held
    lanes = slots * members
    group = 2 * slots
    lane = lax.broadcasted_iota(jnp.int32, (slots, lanes), 1)
    own = lane // members == lax.broadcasted_iota(jnp.int32, (slots, lanes), 0)
    for g in range(held // group):
        weights = weights_ref[g * group * slots : (g + 1) * group * slots, :]
        values = values_ref[g * group * members : (g + 1) * group * members, :]
        every = lax.dot_general(
            weights, values, (((1,), (1,)), ((), ())), preferred_element_type=jnp.float32
        )
        rows = []
        for p in range(group):
            part = every[p * slots : (p + 1) * slots, p // slots * lanes : (p // slots + 1) * lanes]
            turn = (-(p % slots) * members) % lanes
            part = pltpu.roll(part, turn, 1) if turn else part
            part = pltpu.roll(part, 0, 1, stride=members, stride_axis=0)
            rows.append(jnp.sum(jnp.where(own, part, 0.0), axis=0, keepdims=True))
        t_ref[g * group : (g + 1) * group, :] = jnp.concatenate(rows, axis=0)
    count = to_column(count_ref[...].astype(jnp.float32), held)
    slot = (lax.broadcasted_iota(jnp.int32, (held, lanes), 1) // members).astype(jnp.float32)
    terms = jnp.where(slot < count, t_ref[...], 0.0)
    payload = jnp.concatenate(thirds(terms), axis=1).astype(jnp.bfloat16)

    owner = owner_ref[...].astype(jnp.float32)
    square = (held, held)
    before = lax.broadcasted_iota(jnp.int32, square, 0) < lax.broadcasted_iota(jnp.int32, square, 1)
    shared = (to_column(owner, held) == owner) & before
    rank = jnp.sum(jnp.where(shared, 1.0, 0.0), axis=0, keepdims=True)
    devices = out_ref.shape[0]
    device = lax.broadcasted_iota(jnp.int32, (devices, held), 0).astype(jnp.float32)
    mine = jnp.where(device == owner, 1.0, 0.0)
    index = index_ref[...].astype(jnp.float32)
    indices = []
    for k in range(capacity):
        ranked = jnp.where(rank == k, 1.0, 0.0)
        table = (mine * ranked).astype(jnp.bfloat16)
        placed = jnp.dot(table, payload, preferred_element_type=jnp.float32)
        out_ref[:, k * lanes : (k + 1) * lanes] = (
            placed[:, :lanes] + placed[:, lanes : 2 * lanes]
        ) + placed[:, 2 * lanes :]
        indices.append(index * ranked)
    indices.append(jnp.zeros((lanes - capacity * slots, held), jnp.float32))
    out_ref[:, capacity * lanes :] = lax.dot_general(
        mine.astype(jnp.bfloat16),
        jnp.concatenate(indices, axis=0).astype(jnp.bfloat16),
        (((1,), (1,)), ((), ())),
        preferred_element_type=jnp.float32,
    )


def terms_of(values, weights, index, count, owner, devices, capacity):
    slots, held = index.shape
    lanes = slots * (values.shape[0] // held)
    return pl.pallas_call(
        functools.partial(terms_body, capacity),
        out_shape=jax.ShapeDtypeStruct((devices, (capacity + 1) * lanes), jnp.float32),
        in_specs=[pl.BlockSpec(memory_space=VMEM)] * 5,
        out_specs=pl.BlockSpec(memory_space=VMEM),
        scratch_shapes=[pltpu.VMEM((held, lanes), jnp.float32)],
        compiler_params=pltpu.CompilerParams(vmem_limit_bytes=8 * MIB),
        cost_estimate=pl.CostEstimate(flops=10**9, bytes_accessed=10**6, transcendentals=0),
        name="terms",
    )(values, weights, index, count, owner)


def gather_body(capacity, slots, message_ref, z_ref, rhs_ref, copies_ref):
    devices = message_ref.shape[0]
    members, width = rhs_ref.shape
    lanes = slots * members
    index = jnp.transpose(message_ref[:, capacity * lanes :])
    station = lax.broadcasted_iota(jnp.int32, (width, devices), 0).astype(jnp.float32)
    total = jnp.zeros((3 * members, width), jnp.float32)
    for k in range(capacity):
        terms = jnp.transpose(message_ref[:, k * lanes : (k + 1) * lanes])
        split = [part.astype(jnp.bfloat16) for part in thirds(terms)]
        for s in range(slots):
            at = k * slots + s
            here = jnp.where(station == index[at : at + 1, :], 1.0, 0.0).astype(jnp.bfloat16)
            left = jnp.concatenate([p[s * members : (s + 1) * members] for p in split], axis=0)
            total += lax.dot_general(
                left, here, (((1,), (1,)), ((), ())), preferred_element_type=jnp.float32
            )
    rhs = total[:members] + (total[members : 2 * members] + total[2 * members :])
    rhs_ref[...] = rhs
    z = z_ref[...]
    for r in range(copies_ref.shape[0]):
        copies_ref[r, : z.shape[0]] = z
        copies_ref[r, z.shape[0] :] = rhs


def gather_terms(message, z, members, copies, capacity, slots):
    feats, width = z.shape
    return pl.pallas_call(
        functools.partial(gather_body, capacity, slots),
        out_shape=[
            jax.ShapeDtypeStruct((members, width), jnp.float32),
            jax.ShapeDtypeStruct((copies, feats + members, width), jnp.float32),
        ],
        in_specs=[pl.BlockSpec(memory_space=VMEM)] * 2,
        out_specs=[pl.BlockSpec(memory_space=VMEM)] * 2,
        compiler_params=pltpu.CompilerParams(vmem_limit_bytes=8 * MIB),
        cost_estimate=pl.CostEstimate(flops=10**9, bytes_accessed=10**6, transcendentals=0),
        name="gather",
    )(message, z)


def total_body(shares_ref, v_ref, nugget_ref, out_ref, copies_ref):
    total = nugget_ref[...] * v_ref[...]
    for c in range(shares_ref.shape[0]):
        total += shares_ref[c]
    out_ref[...] = total
    for r in range(copies_ref.shape[0]):
        copies_ref[r] = total


def total_of(shares, v, nugget, copies):
    return pl.pallas_call(
        total_body,
        out_shape=[
            jax.ShapeDtypeStruct(v.shape, jnp.float32),
            jax.ShapeDtypeStruct((copies,) + v.shape, jnp.float32),
        ],
        in_specs=[pl.BlockSpec(memory_space=VMEM)] * 3,
        out_specs=[pl.BlockSpec(memory_space=VMEM)] * 2,
        compiler_params=pltpu.CompilerParams(vmem_limit_bytes=4 * MIB),
        name="total",
    )(shares, v, nugget)


def guess_of(norm, energy):
    usable = energy > 0.5 * norm
    return jnp.where(usable, norm / jnp.where(usable, energy, 1.0), 0.0)


def close_body(shares_ref, rhs_ref, first_ref, nugget_ref, second_ref, sums_ref):
    rhs, first = rhs_ref[...], first_ref[...]
    second = nugget_ref[...] * first
    for c in range(shares_ref.shape[0]):
        second += shares_ref[c]
    second_ref[...] = second

    def dot(a, b):
        return jnp.sum(a * b, axis=1, keepdims=True)

    norm, energy = dot(rhs, rhs), dot(rhs, first)
    guess = guess_of(norm, energy)
    resid = rhs - guess * first
    along = first - guess * second
    sums = [
        norm,
        energy,
        dot(resid, resid),
        dot(resid, first),
        dot(first, first),
        dot(resid, along),
        dot(resid, second) + dot(first, along),
        dot(first, second),
    ]
    members = rhs.shape[0]
    shape = (members, len(sums) * members)
    row = lax.broadcasted_iota(jnp.int32, shape, 0)
    lane = lax.broadcasted_iota(jnp.int32, shape, 1)
    spaced = jnp.zeros(shape, jnp.float32)
    for at, column in enumerate(sums):
        here = lane == row + at * members
        spaced += jnp.where(here, jnp.broadcast_to(column, shape), 0.0)
    sums_ref[...] = jnp.sum(spaced, axis=0, keepdims=True)


def close(shares, rhs, first, nugget):
    members = rhs.shape[0]
    return pl.pallas_call(
        close_body,
        out_shape=[
            jax.ShapeDtypeStruct(rhs.shape, jnp.float32),
            jax.ShapeDtypeStruct((1, 8 * members), jnp.float32),
        ],
        in_specs=[pl.BlockSpec(memory_space=VMEM)] * 4,
        out_specs=[pl.BlockSpec(memory_space=VMEM)] * 2,
        compiler_params=pltpu.CompilerParams(vmem_limit_bytes=4 * MIB),
        name="close",
    )(shares, rhs, first, nugget)


def finish_body(sums_ref, rhs_ref, first_ref, second_ref, solved_ref, residual_ref):
    rhs, first, second = rhs_ref[...], first_ref[...], second_ref[...]
    members = rhs.shape[0]
    norm, energy, rr, rf, ff, ra, rs, fs = (
        sums_ref[:, q * members : (q + 1) * members] for q in range(8)
    )

    def over(x):
        return jnp.sum(x, axis=0, keepdims=True)

    norm0 = over(norm)
    alpha0 = norm0 / over(energy)
    shift = alpha0 - guess_of(norm, energy)
    norm1 = over(rr - shift * (2.0 * rf - shift * ff))
    energy1 = over(ra - shift * (rs - shift * fs))
    ratio = norm1 / norm0
    alpha1 = norm1 / (energy1 - ratio * norm1 / alpha0)
    shape = (members, members)
    same = lax.broadcasted_iota(jnp.int32, shape, 0) == lax.broadcasted_iota(jnp.int32, shape, 1)

    def column(x):
        return jnp.sum(jnp.where(same, jnp.broadcast_to(x, shape), 0.0), axis=1, keepdims=True)

    alpha0, alpha1, ratio = column(alpha0), column(alpha1), column(ratio)
    residual = rhs - alpha0 * first
    direction = residual + ratio * rhs
    along = (first - alpha0 * second) + ratio * first
    solved_ref[...] = alpha0 * rhs + alpha1 * direction
    residual_ref[...] = residual - alpha1 * along


def finish(sums, rhs, first, second):
    return pl.pallas_call(
        finish_body,
        out_shape=[jax.ShapeDtypeStruct(rhs.shape, jnp.float32)] * 2,
        in_specs=[pl.BlockSpec(memory_space=VMEM)] * 4,
        out_specs=[pl.BlockSpec(memory_space=VMEM)] * 2,
        compiler_params=pltpu.CompilerParams(vmem_limit_bytes=4 * MIB),
        name="finish",
    )(sums, rhs, first, second)


def exchange(pieces, axes):
    return lax.all_to_all(pieces, axes, split_axis=0, concat_axis=0, tiled=True)


def local(
    covariates, lengthscale, nugget, patch_values, patch_weights, block_index, slot_count, owner
):
    devices = lax.axis_size(ALL)
    held, members, cells = patch_values.shape
    slots = patch_weights.shape[1]
    stations = nugget.shape[0]
    capacity = max(2, 2 * held // devices)

    z = covariates / lengthscale[:, None]
    zi = spread(z, COL)
    message = terms_of(
        patch_values.reshape(held * members, cells),
        patch_weights.reshape(held * slots, cells),
        block_index.T,
        slot_count[None, :],
        owner.T,
        devices,
        capacity,
    )
    zi, message = lax.optimization_barrier((zi, message))
    message = exchange(message, ALL)
    rhs, copies = gather_terms(message, z, members, lax.axis_size(ROW), capacity, slots)
    nugget = nugget[None, :]
    high, low, partial_value = build_and_product(exchange(copies, ROW), zi)
    shares = exchange(partial_value, COL)
    first, copies = total_of(shares, rhs, nugget, lax.axis_size(ROW))
    shares = exchange(kernel_product(exchange(copies, ROW), high, low), COL)
    second, sums = close(shares, rhs, first, nugget)
    copies = jnp.broadcast_to(sums[None], (devices,) + sums.shape)
    sums = exchange(copies, ALL).reshape(devices, sums.shape[1])
    return finish(sums, rhs, first, second)


def solution(mesh):
    torus = Mesh(mesh.devices.reshape(4, 2, 4, 4), ALL)
    placed = (
        P(None, ALL),
        P(),
        P(ALL),
        P(ALL, None, None),
        P(ALL, None, None),
        P(ALL, None),
        P(ALL),
        P(ALL, None),
    )
    return jax.shard_map(
        local,
        mesh=torus,
        in_specs=placed,
        out_specs=(P(None, ALL), P(None, ALL)),
        check_vma=False,
    )
```

```python
import functools
import math

import jax
import jax.numpy as jnp
from jax import lax
from jax.experimental import pallas as pl
from jax.experimental.pallas import tpu as pltpu
from jax.sharding import Mesh
from jax.sharding import PartitionSpec as P

ALL = ("row_0", "row_1", "col_0", "col_1")
COL = ("col_0", "col_1")
ROW = ("row_0", "row_1")

LN2 = math.log(2.0)
SCALE = math.sqrt(5.0) / LN2
FACTOR = LN2 * LN2 / 3.0
LINEAR = 3.0 / LN2
CONST = 3.0 / (LN2 * LN2)
TINY = 1e-30
TALL, WIDE = 512, 256
VMEM = pltpu.MemorySpace.VMEM
HBM = pltpu.MemorySpace.HBM
MIB = 1 << 20


def rotate(x, axis, by):
    size = lax.axis_size(axis)
    return lax.ppermute(x, axis, [(i, (i + by) % size) for i in range(size)])


def ring(x, axis):
    return [rotate(x, axis, by) for by in range(1, lax.axis_size(axis))]


def halves(x):
    high = x.astype(jnp.bfloat16).astype(jnp.float32)
    return high, x - high


def thirds(x):
    high, rest = halves(x)
    middle, low = halves(rest)
    return high, middle, low


def features(z, left):
    high, middle, low = thirds(z)
    norm = jnp.sum(z * z, axis=0, keepdims=True)
    n_high, n_middle, n_low = thirds(norm)
    row = lax.broadcasted_iota(jnp.int32, z.shape, 0)
    base = 0 if left else 3
    rest = jnp.zeros_like(z)
    for at, part in ((base, n_high), (base + 1, n_middle), (base + 2, n_low)):
        rest = jnp.where(row == at, jnp.broadcast_to(part, z.shape), rest)
    rest = jnp.where((row >= 3 - base) & (row < 6 - base), 1.0, rest)
    if left:
        parts = [high, high, high, middle, middle, low]
    else:
        parts = [-2.0 * part for part in (high, middle, low, high, middle, high)]
    return jnp.concatenate(parts + [rest, jnp.zeros_like(z)], axis=0)


def value_of(squared):
    squared = jnp.maximum(squared, TINY)
    root = squared * lax.rsqrt(squared)
    return (squared + (LINEAR * root + CONST)) * jnp.exp2(-root)


def split_vector(v_ref, first, vv_ref):
    width = v_ref.shape[2]
    members = vv_ref.shape[0] // 2
    for r in range(v_ref.shape[0]):
        high, low = halves(v_ref[r, first : first + members])
        columns = slice(r * width, (r + 1) * width)
        vv_ref[:members, columns] = high.astype(jnp.bfloat16)
        vv_ref[members:, columns] = low.astype(jnp.bfloat16)


def build_body(
    zv_ref, fi_ref, high_ref, low_ref, out_ref, fj_ref, vv_ref, acc_ref, ahead_ref
):
    members, width = out_ref.shape[1:]
    feats = zv_ref.shape[1] - members
    for r in range(zv_ref.shape[0]):
        block = features(zv_ref[r, :feats] * SCALE, True)
        fj_ref[r * width : (r + 1) * width, :] = jnp.transpose(block.astype(jnp.bfloat16))
    split_vector(zv_ref, feats, vv_ref)
    acc_ref[...] = jnp.zeros_like(acc_ref)
    tall, wide = TALL, WIDE
    tiles, steps = fi_ref.shape[1] // wide, fj_ref.shape[0] // tall

    def place(step, tile):
        rows = pl.ds(pl.multiple_of(step * tall, tall), tall)
        return rows, slice(tile * wide, (tile + 1) * wide)

    def squares(step, tile):
        rows, columns = place(step, tile)
        return jnp.dot(fj_ref[rows, :], fi_ref[:, columns], preferred_element_type=jnp.float32)

    ahead_ref[...] = squares(0, 0)

    @pl.loop(0, steps)
    def _(step):
        squared = ahead_ref[...]
        for tile in range(tiles):
            if tile + 1 < tiles:
                ahead = squares(step, tile + 1)
            else:
                ahead = squares(jnp.minimum(step + 1, steps - 1), 0)
            rows, columns = place(step, tile)
            value = value_of(squared)
            high = value.astype(jnp.bfloat16)
            low = (value - high.astype(jnp.float32)).astype(jnp.bfloat16)
            high_ref[rows, columns] = high
            low_ref[rows, columns] = low
            vv = vv_ref[:, rows]
            acc_ref[:, columns] += jnp.dot(
                vv, high, preferred_element_type=jnp.float32
            ) + jnp.dot(vv, low, preferred_element_type=jnp.float32)
            squared = ahead
        ahead_ref[...] = squared

    for c in range(out_ref.shape[0]):
        columns = slice(c * width, (c + 1) * width)
        out_ref[c] = FACTOR * (acc_ref[:members, columns] + acc_ref[members:, columns])


def build_and_product(zv, fi, members):
    width = zv.shape[2]
    rows, columns = zv.shape[0] * width, fi.shape[1]
    return pl.pallas_call(
        build_body,
        out_shape=[pltpu.VMEM((rows, columns), jnp.bfloat16)] * 2
        + [jax.ShapeDtypeStruct((columns // width, members, width), jnp.float32)],
        in_specs=[pl.BlockSpec(memory_space=VMEM)] * 2,
        out_specs=[pl.BlockSpec(memory_space=VMEM)] * 3,
        scratch_shapes=[
            pltpu.VMEM((rows, fi.shape[0]), jnp.bfloat16),
            pltpu.VMEM((2 * members, rows), jnp.bfloat16),
            pltpu.VMEM((2 * members, columns), jnp.float32),
            pltpu.VMEM((TALL, WIDE), jnp.float32),
        ],
        compiler_params=pltpu.CompilerParams(vmem_limit_bytes=12 * MIB),
        cost_estimate=pl.CostEstimate(
            flops=40 * rows * columns, bytes_accessed=4 * rows * columns, transcendentals=0
        ),
        name="build",
    )(zv, fi)


def product_body(v_ref, high_ref, low_ref, out_ref, vv_ref):
    _, members, width = v_ref.shape
    split_vector(v_ref, 0, vv_ref)
    vv = vv_ref[...]
    both = jnp.dot(vv, high_ref[...], preferred_element_type=jnp.float32)
    both += jnp.dot(vv, low_ref[...], preferred_element_type=jnp.float32)
    total = FACTOR * (both[:members] + both[members:])
    for c in range(out_ref.shape[0]):
        out_ref[c] = total[:, c * width : (c + 1) * width]


def kernel_product(v, high, low):
    _, members, width = v.shape
    rows, columns = high.shape
    return pl.pallas_call(
        product_body,
        out_shape=jax.ShapeDtypeStruct((columns // width, members, width), jnp.float32),
        in_specs=[pl.BlockSpec(memory_space=VMEM)] * 3,
        out_specs=pl.BlockSpec(memory_space=VMEM),
        scratch_shapes=[pltpu.VMEM((2 * members, rows), jnp.bfloat16)],
        compiler_params=pltpu.CompilerParams(vmem_limit_bytes=12 * MIB),
        cost_estimate=pl.CostEstimate(
            flops=128 * rows * columns, bytes_accessed=4 * rows * columns, transcendentals=0
        ),
        name="product",
    )(v, high, low)


def to_column(row, size):
    shape = (size, row.shape[1])
    same = lax.broadcasted_iota(jnp.int32, shape, 0) == lax.broadcasted_iota(jnp.int32, shape, 1)
    return jnp.sum(jnp.where(same, jnp.broadcast_to(row, shape), 0.0), axis=1, keepdims=True)


def terms_body(capacity, *refs):
    sources, (out_ref, z_ref, nugget_out_ref) = refs[:8], refs[8:11]
    t_ref, held_refs, sems = refs[11], refs[12:20], refs[20]
    copies = [
        pltpu.make_async_copy(source, held_ref, sems.at[i])
        for i, (source, held_ref) in enumerate(zip(sources, held_refs))
    ]
    for copy in copies:
        copy.start()
    values_ref, weights_ref, index_ref, count_ref, owner_ref, cov_ref, scale_ref, nugget_ref = held_refs
    slots, held = index_ref.shape
    members = values_ref.shape[0] // held
    lanes = slots * members
    group = 2 * slots

    for copy in copies[2:]:
        copy.wait()
    z_ref[...] = cov_ref[...] / to_column(scale_ref[...], cov_ref.shape[0])
    nugget_out_ref[...] = nugget_ref[...]
    owner = owner_ref[...].astype(jnp.float32)
    square = (held, held)
    before = lax.broadcasted_iota(jnp.int32, square, 0) < lax.broadcasted_iota(jnp.int32, square, 1)
    shared = (to_column(owner, held) == owner) & before
    rank = jnp.sum(jnp.where(shared, 1.0, 0.0), axis=0, keepdims=True)
    devices = out_ref.shape[0]
    device = lax.broadcasted_iota(jnp.int32, (devices, held), 0).astype(jnp.float32)
    mine = jnp.where(device == owner, 1.0, 0.0)
    count = to_column(count_ref[...].astype(jnp.float32), held)
    index = index_ref[...].astype(jnp.float32)
    ranked = [jnp.where(rank == k, 1.0, 0.0) for k in range(capacity)]
    indices = [index * r for r in ranked]
    indices.append(jnp.zeros((lanes - capacity * slots, held), jnp.float32))
    out_ref[:, capacity * lanes :] = lax.dot_general(
        mine.astype(jnp.bfloat16),
        jnp.concatenate(indices, axis=0).astype(jnp.bfloat16),
        (((1,), (1,)), ((), ())),
        preferred_element_type=jnp.float32,
    )

    for copy in copies[:2]:
        copy.wait()
    lane = lax.broadcasted_iota(jnp.int32, (slots, lanes), 1)
    own = lane // members == lax.broadcasted_iota(jnp.int32, (slots, lanes), 0)
    for g in range(held // group):
        weights = weights_ref[g * group * slots : (g + 1) * group * slots, :]
        values = values_ref[g * group * members : (g + 1) * group * members, :]
        every = lax.dot_general(
            weights, values, (((1,), (1,)), ((), ())), preferred_element_type=jnp.float32
        )
        rows = []
        for p in range(group):
            part = every[p * slots : (p + 1) * slots, p // slots * lanes : (p // slots + 1) * lanes]
            turn = (-(p % slots) * members) % lanes
            part = pltpu.roll(part, turn, 1) if turn else part
            part = pltpu.roll(part, 0, 1, stride=members, stride_axis=0)
            rows.append(jnp.sum(jnp.where(own, part, 0.0), axis=0, keepdims=True))
        t_ref[g * group : (g + 1) * group, :] = jnp.concatenate(rows, axis=0)
    slot = (lax.broadcasted_iota(jnp.int32, (held, lanes), 1) // members).astype(jnp.float32)
    terms = jnp.where(slot < count, t_ref[...], 0.0)
    payload = jnp.concatenate(thirds(terms), axis=1).astype(jnp.bfloat16)
    for k in range(capacity):
        table = (mine * ranked[k]).astype(jnp.bfloat16)
        placed = jnp.dot(table, payload, preferred_element_type=jnp.float32)
        out_ref[:, k * lanes : (k + 1) * lanes] = (
            placed[:, :lanes] + placed[:, lanes : 2 * lanes]
        ) + placed[:, 2 * lanes :]


def terms_of(args, devices, capacity):
    values, _, index, _, _, covariates, _, nugget = args
    slots, held = index.shape
    lanes = slots * (values.shape[0] // held)
    return pl.pallas_call(
        functools.partial(terms_body, capacity),
        out_shape=[
            jax.ShapeDtypeStruct((devices, (capacity + 1) * lanes), jnp.float32),
            jax.ShapeDtypeStruct(covariates.shape, jnp.float32),
            jax.ShapeDtypeStruct(nugget.shape, jnp.float32),
        ],
        in_specs=[pl.BlockSpec(memory_space=HBM)] * len(args),
        out_specs=[pl.BlockSpec(memory_space=VMEM)] * 3,
        scratch_shapes=[pltpu.VMEM((held, lanes), jnp.float32)]
        + [pltpu.VMEM(x.shape, x.dtype) for x in args]
        + [pltpu.SemaphoreType.DMA((len(args),))],
        compiler_params=pltpu.CompilerParams(vmem_limit_bytes=8 * MIB),
        cost_estimate=pl.CostEstimate(flops=10**9, bytes_accessed=10**6, transcendentals=0),
        name="terms",
    )(*(pltpu.with_memory_space_constraint(x, HBM) for x in args))


def place_body(*refs):
    pieces, fi_ref = refs[:-1], refs[-1]
    width = pieces[0].shape[2]
    outer, inner = lax.axis_index(COL[0]), lax.axis_index(COL[1])
    sides = [lax.axis_size(name) for name in COL]
    at = 0
    for ref in pieces:
        for n in range(ref.shape[0]):
            by_inner, by_outer = at // sides[0], at % sides[0]
            source = (outer - by_outer + sides[0]) % sides[0] * sides[1]
            source += (inner - by_inner + sides[1]) % sides[1]
            columns = pl.ds(pl.multiple_of(source * width, width), width)
            fi_ref[:, columns] = features(ref[n] * SCALE, False).astype(jnp.bfloat16)
            at += 1


def place(pieces):
    width = pieces[0].shape[2]
    blocks = sum(piece.shape[0] for piece in pieces)
    return pl.pallas_call(
        place_body,
        out_shape=jax.ShapeDtypeStruct((128, blocks * width), jnp.bfloat16),
        in_specs=[pl.BlockSpec(memory_space=VMEM)] * len(pieces),
        out_specs=pl.BlockSpec(memory_space=VMEM),
        compiler_params=pltpu.CompilerParams(vmem_limit_bytes=4 * MIB),
        cost_estimate=pl.CostEstimate(flops=10**9, bytes_accessed=10**6, transcendentals=0),
        name="place",
    )(*pieces)


def gather_body(capacity, slots, message_ref, z_ref, rhs_ref, copies_ref):
    devices = message_ref.shape[0]
    members, width = rhs_ref.shape
    lanes = slots * members
    index = jnp.transpose(message_ref[:, capacity * lanes :])
    station = lax.broadcasted_iota(jnp.int32, (width, devices), 0).astype(jnp.float32)
    total = jnp.zeros((3 * members, width), jnp.float32)
    for k in range(capacity):
        terms = jnp.transpose(message_ref[:, k * lanes : (k + 1) * lanes])
        split = [part.astype(jnp.bfloat16) for part in thirds(terms)]
        for s in range(slots):
            at = k * slots + s
            here = jnp.where(station == index[at : at + 1, :], 1.0, 0.0).astype(jnp.bfloat16)
            left = jnp.concatenate([p[s * members : (s + 1) * members] for p in split], axis=0)
            total += lax.dot_general(
                left, here, (((1,), (1,)), ((), ())), preferred_element_type=jnp.float32
            )
    rhs = total[:members] + (total[members : 2 * members] + total[2 * members :])
    rhs_ref[...] = rhs
    z = z_ref[...]
    for r in range(copies_ref.shape[0]):
        copies_ref[r, : z.shape[0]] = z
        copies_ref[r, z.shape[0] :] = rhs


def gather_terms(message, z, members, copies, capacity, slots):
    feats, width = z.shape
    return pl.pallas_call(
        functools.partial(gather_body, capacity, slots),
        out_shape=[
            jax.ShapeDtypeStruct((members, width), jnp.float32),
            jax.ShapeDtypeStruct((copies, feats + members, width), jnp.float32),
        ],
        in_specs=[pl.BlockSpec(memory_space=VMEM)] * 2,
        out_specs=[pl.BlockSpec(memory_space=VMEM)] * 2,
        compiler_params=pltpu.CompilerParams(vmem_limit_bytes=8 * MIB),
        cost_estimate=pl.CostEstimate(flops=10**9, bytes_accessed=10**6, transcendentals=0),
        name="gather",
    )(message, z)


def total_body(shares_ref, v_ref, nugget_ref, out_ref, copies_ref):
    total = nugget_ref[...] * v_ref[...]
    for c in range(shares_ref.shape[0]):
        total += shares_ref[c]
    out_ref[...] = total
    for r in range(copies_ref.shape[0]):
        copies_ref[r] = total


def total_of(shares, v, nugget, copies):
    return pl.pallas_call(
        total_body,
        out_shape=[
            jax.ShapeDtypeStruct(v.shape, jnp.float32),
            jax.ShapeDtypeStruct((copies,) + v.shape, jnp.float32),
        ],
        in_specs=[pl.BlockSpec(memory_space=VMEM)] * 3,
        out_specs=[pl.BlockSpec(memory_space=VMEM)] * 2,
        compiler_params=pltpu.CompilerParams(vmem_limit_bytes=4 * MIB),
        name="total",
    )(shares, v, nugget)


def guess_of(norm, energy):
    usable = energy > 0.5 * norm
    return jnp.where(usable, norm / jnp.where(usable, energy, 1.0), 0.0)


def close_body(shares_ref, rhs_ref, first_ref, nugget_ref, second_ref, sums_ref):
    rhs, first = rhs_ref[...], first_ref[...]
    second = nugget_ref[...] * first
    for c in range(shares_ref.shape[0]):
        second += shares_ref[c]
    second_ref[...] = second

    def dot(a, b):
        return jnp.sum(a * b, axis=1, keepdims=True)

    norm, energy = dot(rhs, rhs), dot(rhs, first)
    guess = guess_of(norm, energy)
    resid = rhs - guess * first
    along = first - guess * second
    sums = [
        norm,
        energy,
        dot(resid, resid),
        dot(resid, first),
        dot(first, first),
        dot(resid, along),
        dot(resid, second) + dot(first, along),
        dot(first, second),
    ]
    members = rhs.shape[0]
    shape = (members, len(sums) * members)
    row = lax.broadcasted_iota(jnp.int32, shape, 0)
    lane = lax.broadcasted_iota(jnp.int32, shape, 1)
    spaced = jnp.zeros(shape, jnp.float32)
    for at, column in enumerate(sums):
        here = lane == row + at * members
        spaced += jnp.where(here, jnp.broadcast_to(column, shape), 0.0)
    sums_ref[...] = jnp.sum(spaced, axis=0, keepdims=True)


def close(shares, rhs, first, nugget):
    members = rhs.shape[0]
    return pl.pallas_call(
        close_body,
        out_shape=[
            jax.ShapeDtypeStruct(rhs.shape, jnp.float32),
            jax.ShapeDtypeStruct((1, 8 * members), jnp.float32),
        ],
        in_specs=[pl.BlockSpec(memory_space=VMEM)] * 4,
        out_specs=[pl.BlockSpec(memory_space=VMEM)] * 2,
        compiler_params=pltpu.CompilerParams(vmem_limit_bytes=4 * MIB),
        name="close",
    )(shares, rhs, first, nugget)


def finish_body(sums_ref, rhs_ref, first_ref, second_ref, solved_ref, residual_ref):
    rhs, first, second = rhs_ref[...], first_ref[...], second_ref[...]
    members = rhs.shape[0]
    norm, energy, rr, rf, ff, ra, rs, fs = (
        sums_ref[:, q * members : (q + 1) * members] for q in range(8)
    )

    def over(x):
        return jnp.sum(x, axis=0, keepdims=True)

    norm0 = over(norm)
    alpha0 = norm0 / over(energy)
    shift = alpha0 - guess_of(norm, energy)
    norm1 = over(rr - shift * (2.0 * rf - shift * ff))
    energy1 = over(ra - shift * (rs - shift * fs))
    ratio = norm1 / norm0
    alpha1 = norm1 / (energy1 - ratio * norm1 / alpha0)
    shape = (members, members)
    same = lax.broadcasted_iota(jnp.int32, shape, 0) == lax.broadcasted_iota(jnp.int32, shape, 1)

    def column(x):
        return jnp.sum(jnp.where(same, jnp.broadcast_to(x, shape), 0.0), axis=1, keepdims=True)

    alpha0, alpha1, ratio = column(alpha0), column(alpha1), column(ratio)
    residual = rhs - alpha0 * first
    direction = residual + ratio * rhs
    along = (first - alpha0 * second) + ratio * first
    solved_ref[...] = alpha0 * rhs + alpha1 * direction
    residual_ref[...] = residual - alpha1 * along


def finish(sums, rhs, first, second):
    return pl.pallas_call(
        finish_body,
        out_shape=[jax.ShapeDtypeStruct(rhs.shape, jnp.float32)] * 2,
        in_specs=[pl.BlockSpec(memory_space=VMEM)] * 4,
        out_specs=[pl.BlockSpec(memory_space=VMEM)] * 2,
        compiler_params=pltpu.CompilerParams(vmem_limit_bytes=4 * MIB),
        name="finish",
    )(sums, rhs, first, second)


def exchange(pieces, axes):
    return lax.all_to_all(pieces, axes, split_axis=0, concat_axis=0, tiled=True)


def local(
    covariates, lengthscale, nugget, patch_values, patch_weights, block_index, slot_count, owner
):
    devices = lax.axis_size(ALL)
    held, members, cells = patch_values.shape
    slots = patch_weights.shape[1]
    capacity = max(2, 2 * held // devices)

    message, z, nugget = terms_of(
        (
            patch_values.reshape(held * members, cells),
            patch_weights.reshape(held * slots, cells),
            block_index.T,
            slot_count[None, :],
            owner.T,
            covariates,
            lengthscale[None, :],
            nugget[None, :],
        ),
        devices,
        capacity,
    )
    near = [z[None]] + ring(z[None], COL[0])
    far = ring(jnp.concatenate(near), COL[1])
    row_features = place(near + far)
    message = exchange(message, ALL)
    rhs, copies = gather_terms(message, z, members, lax.axis_size(ROW), capacity, slots)
    high, low, partial_value = build_and_product(exchange(copies, ROW), row_features, members)
    shares = exchange(partial_value, COL)
    first, copies = total_of(shares, rhs, nugget, lax.axis_size(ROW))
    shares = exchange(kernel_product(exchange(copies, ROW), high, low), COL)
    second, sums = close(shares, rhs, first, nugget)
    copies = jnp.broadcast_to(sums[None], (devices,) + sums.shape)
    sums = exchange(copies, ALL).reshape(devices, sums.shape[1])
    return finish(sums, rhs, first, second)


def solution(mesh):
    torus = Mesh(mesh.devices.reshape(4, 2, 4, 4), ALL)
    placed = (
        P(None, ALL),
        P(),
        P(ALL),
        P(ALL, None, None),
        P(ALL, None, None),
        P(ALL, None),
        P(ALL),
        P(ALL, None),
    )
    return jax.shard_map(
        local,
        mesh=torus,
        in_specs=placed,
        out_specs=(P(None, ALL), P(None, ALL)),
        check_vma=False,
    )
```

```python
import functools
import math

import jax
import jax.numpy as jnp
from jax import lax
from jax.experimental import pallas as pl
from jax.experimental.pallas import tpu as pltpu
from jax.sharding import Mesh
from jax.sharding import PartitionSpec as P

ALL = ("row_0", "row_1", "col_0", "col_1")
COL = ("col_0", "col_1")
ROW = ("row_0", "row_1")

LN2 = math.log(2.0)
SCALE = math.sqrt(5.0) / LN2
FACTOR = LN2 * LN2 / 3.0
LINEAR = 3.0 / LN2
CONST = 3.0 / (LN2 * LN2)
TINY = 1e-30
TALL, WIDE = 512, 256
VMEM = pltpu.MemorySpace.VMEM
HBM = pltpu.MemorySpace.HBM
MIB = 1 << 20


def rotate(x, axis, by):
    size = lax.axis_size(axis)
    return lax.ppermute(x, axis, [(i, (i + by) % size) for i in range(size)])


def ring(x, axis):
    return [rotate(x, axis, by) for by in range(1, lax.axis_size(axis))]


def halves(x):
    high = x.astype(jnp.bfloat16).astype(jnp.float32)
    return high, x - high


def thirds(x):
    high, rest = halves(x)
    middle, low = halves(rest)
    return high, middle, low


def features(z, left):
    high, middle, low = thirds(z)
    norm = jnp.sum(z * z, axis=0, keepdims=True)
    n_high, n_middle, n_low = thirds(norm)
    row = lax.broadcasted_iota(jnp.int32, z.shape, 0)
    base = 0 if left else 3
    rest = jnp.zeros_like(z)
    for at, part in ((base, n_high), (base + 1, n_middle), (base + 2, n_low)):
        rest = jnp.where(row == at, jnp.broadcast_to(part, z.shape), rest)
    rest = jnp.where((row >= 3 - base) & (row < 6 - base), 1.0, rest)
    if left:
        parts = [high, high, high, middle, middle, low]
    else:
        parts = [-2.0 * part for part in (high, middle, low, high, middle, high)]
    return jnp.concatenate(parts + [rest, jnp.zeros_like(z)], axis=0)


def value_of(squared):
    squared = jnp.maximum(squared, TINY)
    root = squared * lax.rsqrt(squared)
    return (squared + (LINEAR * root + CONST)) * jnp.exp2(-root)


def split_vector(v_ref, vv_ref):
    width = v_ref.shape[2]
    members = vv_ref.shape[0] // 2
    for r in range(v_ref.shape[0]):
        high, low = halves(v_ref[r])
        columns = slice(r * width, (r + 1) * width)
        vv_ref[:members, columns] = high.astype(jnp.bfloat16)
        vv_ref[members:, columns] = low.astype(jnp.bfloat16)


def build_body(v_ref, fi_ref, fj_ref, high_ref, low_ref, out_ref, vv_ref, acc_ref, ahead_ref):
    members, width = out_ref.shape[1:]
    split_vector(v_ref, vv_ref)
    acc_ref[...] = jnp.zeros_like(acc_ref)
    tall, wide = TALL, WIDE
    tiles, steps = fi_ref.shape[1] // wide, fj_ref.shape[0] // tall

    def place(step, tile):
        rows = pl.ds(pl.multiple_of(step * tall, tall), tall)
        return rows, slice(tile * wide, (tile + 1) * wide)

    def squares(step, tile):
        rows, columns = place(step, tile)
        return jnp.dot(fj_ref[rows, :], fi_ref[:, columns], preferred_element_type=jnp.float32)

    ahead_ref[...] = squares(0, 0)

    @pl.loop(0, steps)
    def _(step):
        squared = ahead_ref[...]
        for tile in range(tiles):
            if tile + 1 < tiles:
                ahead = squares(step, tile + 1)
            else:
                ahead = squares(jnp.minimum(step + 1, steps - 1), 0)
            rows, columns = place(step, tile)
            value = value_of(squared)
            high = value.astype(jnp.bfloat16)
            low = (value - high.astype(jnp.float32)).astype(jnp.bfloat16)
            high_ref[rows, columns] = high
            low_ref[rows, columns] = low
            vv = vv_ref[:, rows]
            acc_ref[:, columns] += jnp.dot(
                vv, high, preferred_element_type=jnp.float32
            ) + jnp.dot(vv, low, preferred_element_type=jnp.float32)
            squared = ahead
        ahead_ref[...] = squared

    for c in range(out_ref.shape[0]):
        columns = slice(c * width, (c + 1) * width)
        out_ref[c] = FACTOR * (acc_ref[:members, columns] + acc_ref[members:, columns])


def build_and_product(v, fi, fj):
    members, width = v.shape[1:]
    rows, columns = fj.shape[0], fi.shape[1]
    return pl.pallas_call(
        build_body,
        out_shape=[pltpu.VMEM((rows, columns), jnp.bfloat16)] * 2
        + [jax.ShapeDtypeStruct((columns // width, members, width), jnp.float32)],
        in_specs=[pl.BlockSpec(memory_space=VMEM)] * 3,
        out_specs=[pl.BlockSpec(memory_space=VMEM)] * 3,
        scratch_shapes=[
            pltpu.VMEM((2 * members, rows), jnp.bfloat16),
            pltpu.VMEM((2 * members, columns), jnp.float32),
            pltpu.VMEM((TALL, WIDE), jnp.float32),
        ],
        compiler_params=pltpu.CompilerParams(vmem_limit_bytes=12 * MIB),
        cost_estimate=pl.CostEstimate(
            flops=40 * rows * columns, bytes_accessed=4 * rows * columns, transcendentals=0
        ),
        name="build",
    )(v, fi, fj)


def product_body(v_ref, high_ref, low_ref, out_ref, vv_ref):
    _, members, width = v_ref.shape
    split_vector(v_ref, vv_ref)
    vv = vv_ref[...]
    both = jnp.dot(vv, high_ref[...], preferred_element_type=jnp.float32)
    both += jnp.dot(vv, low_ref[...], preferred_element_type=jnp.float32)
    total = FACTOR * (both[:members] + both[members:])
    for c in range(out_ref.shape[0]):
        out_ref[c] = total[:, c * width : (c + 1) * width]


def kernel_product(v, high, low):
    _, members, width = v.shape
    rows, columns = high.shape
    return pl.pallas_call(
        product_body,
        out_shape=jax.ShapeDtypeStruct((columns // width, members, width), jnp.float32),
        in_specs=[pl.BlockSpec(memory_space=VMEM)] * 3,
        out_specs=pl.BlockSpec(memory_space=VMEM),
        scratch_shapes=[pltpu.VMEM((2 * members, rows), jnp.bfloat16)],
        compiler_params=pltpu.CompilerParams(vmem_limit_bytes=12 * MIB),
        cost_estimate=pl.CostEstimate(
            flops=128 * rows * columns, bytes_accessed=4 * rows * columns, transcendentals=0
        ),
        name="product",
    )(v, high, low)


def to_column(row, size):
    shape = (size, row.shape[1])
    same = lax.broadcasted_iota(jnp.int32, shape, 0) == lax.broadcasted_iota(jnp.int32, shape, 1)
    return jnp.sum(jnp.where(same, jnp.broadcast_to(row, shape), 0.0), axis=1, keepdims=True)


def terms_body(capacity, *refs):
    sources, (out_ref, z_ref, nugget_out_ref) = refs[:8], refs[8:11]
    t_ref, held_refs, sems = refs[11], refs[12:20], refs[20]
    copies = [
        pltpu.make_async_copy(source, held_ref, sems.at[i])
        for i, (source, held_ref) in enumerate(zip(sources, held_refs))
    ]
    for copy in copies:
        copy.start()
    values_ref, weights_ref, index_ref, count_ref, owner_ref, cov_ref, scale_ref, nugget_ref = held_refs
    slots, held = index_ref.shape
    members = values_ref.shape[0] // held
    lanes = slots * members
    group = 2 * slots

    for copy in copies[2:]:
        copy.wait()
    z_ref[...] = cov_ref[...] / to_column(scale_ref[...], cov_ref.shape[0])
    nugget_out_ref[...] = nugget_ref[...]
    owner = owner_ref[...].astype(jnp.float32)
    square = (held, held)
    before = lax.broadcasted_iota(jnp.int32, square, 0) < lax.broadcasted_iota(jnp.int32, square, 1)
    shared = (to_column(owner, held) == owner) & before
    rank = jnp.sum(jnp.where(shared, 1.0, 0.0), axis=0, keepdims=True)
    devices = out_ref.shape[0]
    device = lax.broadcasted_iota(jnp.int32, (devices, held), 0).astype(jnp.float32)
    mine = jnp.where(device == owner, 1.0, 0.0)
    count = to_column(count_ref[...].astype(jnp.float32), held)
    index = index_ref[...].astype(jnp.float32)
    ranked = [jnp.where(rank == k, 1.0, 0.0) for k in range(capacity)]
    indices = [index * r for r in ranked]
    indices.append(jnp.zeros((lanes - capacity * slots, held), jnp.float32))
    out_ref[:, capacity * lanes :] = lax.dot_general(
        mine.astype(jnp.bfloat16),
        jnp.concatenate(indices, axis=0).astype(jnp.bfloat16),
        (((1,), (1,)), ((), ())),
        preferred_element_type=jnp.float32,
    )

    for copy in copies[:2]:
        copy.wait()
    lane = lax.broadcasted_iota(jnp.int32, (slots, lanes), 1)
    own = lane // members == lax.broadcasted_iota(jnp.int32, (slots, lanes), 0)
    for g in range(held // group):
        weights = weights_ref[g * group * slots : (g + 1) * group * slots, :]
        values = values_ref[g * group * members : (g + 1) * group * members, :]
        every = lax.dot_general(
            weights, values, (((1,), (1,)), ((), ())), preferred_element_type=jnp.float32
        )
        rows = []
        for p in range(group):
            part = every[p * slots : (p + 1) * slots, p // slots * lanes : (p // slots + 1) * lanes]
            turn = (-(p % slots) * members) % lanes
            part = pltpu.roll(part, turn, 1) if turn else part
            part = pltpu.roll(part, 0, 1, stride=members, stride_axis=0)
            rows.append(jnp.sum(jnp.where(own, part, 0.0), axis=0, keepdims=True))
        t_ref[g * group : (g + 1) * group, :] = jnp.concatenate(rows, axis=0)
    slot = (lax.broadcasted_iota(jnp.int32, (held, lanes), 1) // members).astype(jnp.float32)
    terms = jnp.where(slot < count, t_ref[...], 0.0)
    payload = jnp.concatenate(thirds(terms), axis=1).astype(jnp.bfloat16)
    for k in range(capacity):
        table = (mine * ranked[k]).astype(jnp.bfloat16)
        placed = jnp.dot(table, payload, preferred_element_type=jnp.float32)
        out_ref[:, k * lanes : (k + 1) * lanes] = (
            placed[:, :lanes] + placed[:, lanes : 2 * lanes]
        ) + placed[:, 2 * lanes :]


def terms_of(args, devices, capacity):
    values, _, index, _, _, covariates, _, nugget = args
    slots, held = index.shape
    lanes = slots * (values.shape[0] // held)
    return pl.pallas_call(
        functools.partial(terms_body, capacity),
        out_shape=[
            jax.ShapeDtypeStruct((devices, (capacity + 1) * lanes), jnp.float32),
            jax.ShapeDtypeStruct(covariates.shape, jnp.float32),
            jax.ShapeDtypeStruct(nugget.shape, jnp.float32),
        ],
        in_specs=[pl.BlockSpec(memory_space=HBM)] * len(args),
        out_specs=[pl.BlockSpec(memory_space=VMEM)] * 3,
        scratch_shapes=[pltpu.VMEM((held, lanes), jnp.float32)]
        + [pltpu.VMEM(x.shape, x.dtype) for x in args]
        + [pltpu.SemaphoreType.DMA((len(args),))],
        compiler_params=pltpu.CompilerParams(vmem_limit_bytes=8 * MIB),
        cost_estimate=pl.CostEstimate(flops=10**9, bytes_accessed=10**6, transcendentals=0),
        name="terms",
    )(*(pltpu.with_memory_space_constraint(x, HBM) for x in args))


def sources(axes, order):
    outer, inner = (lax.axis_index(name) for name in axes)
    sides = [lax.axis_size(name) for name in axes]
    for by_outer, by_inner in order:
        source = (outer - by_outer + sides[0]) % sides[0] * sides[1]
        yield source + (inner - by_inner + sides[1]) % sides[1]


def place_body(count, *refs):
    pieces, (fi_ref, fj_ref) = refs[:-2], refs[-2:]
    width = pieces[0].shape[2]
    blocks = [(ref, n) for ref in pieces[:count] for n in range(ref.shape[0])]
    sides = [lax.axis_size(name) for name in COL]
    order = [(at % sides[0], at // sides[0]) for at in range(len(blocks))]
    for (ref, n), source in zip(blocks, sources(COL, order)):
        columns = pl.ds(pl.multiple_of(source * width, width), width)
        fi_ref[:, columns] = features(ref[n] * SCALE, False).astype(jnp.bfloat16)
    blocks = [(ref, n) for ref in pieces[count:] for n in range(ref.shape[0])]
    sides = [lax.axis_size(name) for name in ROW]
    order = [(at // sides[1], at % sides[1]) for at in range(len(blocks))]
    for (ref, n), source in zip(blocks, sources(ROW, order)):
        rows = pl.ds(pl.multiple_of(source * width, width), width)
        block = features(ref[n] * SCALE, True)
        fj_ref[rows, :] = jnp.transpose(block.astype(jnp.bfloat16))


def place(row_pieces, column_pieces):
    width = row_pieces[0].shape[2]
    rows = sum(piece.shape[0] for piece in row_pieces) * width
    columns = sum(piece.shape[0] for piece in column_pieces) * width
    return pl.pallas_call(
        functools.partial(place_body, len(row_pieces)),
        out_shape=[
            jax.ShapeDtypeStruct((128, rows), jnp.bfloat16),
            jax.ShapeDtypeStruct((columns, 128), jnp.bfloat16),
        ],
        in_specs=[pl.BlockSpec(memory_space=VMEM)] * len(row_pieces + column_pieces),
        out_specs=[pl.BlockSpec(memory_space=VMEM)] * 2,
        compiler_params=pltpu.CompilerParams(vmem_limit_bytes=4 * MIB),
        cost_estimate=pl.CostEstimate(flops=10**9, bytes_accessed=10**6, transcendentals=0),
        name="place",
    )(*row_pieces, *column_pieces)


def gather_body(capacity, slots, message_ref, rhs_ref, copies_ref):
    devices = message_ref.shape[0]
    members, width = rhs_ref.shape
    lanes = slots * members
    index = jnp.transpose(message_ref[:, capacity * lanes :])
    station = lax.broadcasted_iota(jnp.int32, (width, devices), 0).astype(jnp.float32)
    total = jnp.zeros((3 * members, width), jnp.float32)
    for k in range(capacity):
        terms = jnp.transpose(message_ref[:, k * lanes : (k + 1) * lanes])
        split = [part.astype(jnp.bfloat16) for part in thirds(terms)]
        for s in range(slots):
            at = k * slots + s
            here = jnp.where(station == index[at : at + 1, :], 1.0, 0.0).astype(jnp.bfloat16)
            left = jnp.concatenate([p[s * members : (s + 1) * members] for p in split], axis=0)
            total += lax.dot_general(
                left, here, (((1,), (1,)), ((), ())), preferred_element_type=jnp.float32
            )
    rhs = total[:members] + (total[members : 2 * members] + total[2 * members :])
    rhs_ref[...] = rhs
    for r in range(copies_ref.shape[0]):
        copies_ref[r] = rhs


def gather_terms(message, shape, copies, capacity, slots):
    return pl.pallas_call(
        functools.partial(gather_body, capacity, slots),
        out_shape=[
            jax.ShapeDtypeStruct(shape, jnp.float32),
            jax.ShapeDtypeStruct((copies,) + shape, jnp.float32),
        ],
        in_specs=[pl.BlockSpec(memory_space=VMEM)],
        out_specs=[pl.BlockSpec(memory_space=VMEM)] * 2,
        compiler_params=pltpu.CompilerParams(vmem_limit_bytes=8 * MIB),
        cost_estimate=pl.CostEstimate(flops=10**9, bytes_accessed=10**6, transcendentals=0),
        name="gather",
    )(message)


def total_body(shares_ref, v_ref, nugget_ref, out_ref, copies_ref):
    total = nugget_ref[...] * v_ref[...]
    for c in range(shares_ref.shape[0]):
        total += shares_ref[c]
    out_ref[...] = total
    for r in range(copies_ref.shape[0]):
        copies_ref[r] = total


def total_of(shares, v, nugget, copies):
    return pl.pallas_call(
        total_body,
        out_shape=[
            jax.ShapeDtypeStruct(v.shape, jnp.float32),
            jax.ShapeDtypeStruct((copies,) + v.shape, jnp.float32),
        ],
        in_specs=[pl.BlockSpec(memory_space=VMEM)] * 3,
        out_specs=[pl.BlockSpec(memory_space=VMEM)] * 2,
        compiler_params=pltpu.CompilerParams(vmem_limit_bytes=4 * MIB),
        name="total",
    )(shares, v, nugget)


def guess_of(norm, energy):
    usable = energy > 0.5 * norm
    return jnp.where(usable, norm / jnp.where(usable, energy, 1.0), 0.0)


def close_body(shares_ref, rhs_ref, first_ref, nugget_ref, second_ref, sums_ref):
    rhs, first = rhs_ref[...], first_ref[...]
    second = nugget_ref[...] * first
    for c in range(shares_ref.shape[0]):
        second += shares_ref[c]
    second_ref[...] = second

    def dot(a, b):
        return jnp.sum(a * b, axis=1, keepdims=True)

    norm, energy = dot(rhs, rhs), dot(rhs, first)
    guess = guess_of(norm, energy)
    resid = rhs - guess * first
    along = first - guess * second
    sums = [
        norm,
        energy,
        dot(resid, resid),
        dot(resid, first),
        dot(first, first),
        dot(resid, along),
        dot(resid, second) + dot(first, along),
        dot(first, second),
    ]
    members = rhs.shape[0]
    shape = (members, len(sums) * members)
    row = lax.broadcasted_iota(jnp.int32, shape, 0)
    lane = lax.broadcasted_iota(jnp.int32, shape, 1)
    spaced = jnp.zeros(shape, jnp.float32)
    for at, column in enumerate(sums):
        here = lane == row + at * members
        spaced += jnp.where(here, jnp.broadcast_to(column, shape), 0.0)
    sums_ref[...] = jnp.sum(spaced, axis=0, keepdims=True)


def close(shares, rhs, first, nugget):
    members = rhs.shape[0]
    return pl.pallas_call(
        close_body,
        out_shape=[
            jax.ShapeDtypeStruct(rhs.shape, jnp.float32),
            jax.ShapeDtypeStruct((1, 8 * members), jnp.float32),
        ],
        in_specs=[pl.BlockSpec(memory_space=VMEM)] * 4,
        out_specs=[pl.BlockSpec(memory_space=VMEM)] * 2,
        compiler_params=pltpu.CompilerParams(vmem_limit_bytes=4 * MIB),
        name="close",
    )(shares, rhs, first, nugget)


def finish_body(sums_ref, rhs_ref, first_ref, second_ref, solved_ref, residual_ref):
    rhs, first, second = rhs_ref[...], first_ref[...], second_ref[...]
    members = rhs.shape[0]
    norm, energy, rr, rf, ff, ra, rs, fs = (
        sums_ref[:, q * members : (q + 1) * members] for q in range(8)
    )

    def over(x):
        return jnp.sum(x, axis=0, keepdims=True)

    norm0 = over(norm)
    alpha0 = norm0 / over(energy)
    shift = alpha0 - guess_of(norm, energy)
    norm1 = over(rr - shift * (2.0 * rf - shift * ff))
    energy1 = over(ra - shift * (rs - shift * fs))
    ratio = norm1 / norm0
    alpha1 = norm1 / (energy1 - ratio * norm1 / alpha0)
    shape = (members, members)
    same = lax.broadcasted_iota(jnp.int32, shape, 0) == lax.broadcasted_iota(jnp.int32, shape, 1)

    def column(x):
        return jnp.sum(jnp.where(same, jnp.broadcast_to(x, shape), 0.0), axis=1, keepdims=True)

    alpha0, alpha1, ratio = column(alpha0), column(alpha1), column(ratio)
    residual = rhs - alpha0 * first
    direction = residual + ratio * rhs
    along = (first - alpha0 * second) + ratio * first
    solved_ref[...] = alpha0 * rhs + alpha1 * direction
    residual_ref[...] = residual - alpha1 * along


def finish(sums, rhs, first, second):
    return pl.pallas_call(
        finish_body,
        out_shape=[jax.ShapeDtypeStruct(rhs.shape, jnp.float32)] * 2,
        in_specs=[pl.BlockSpec(memory_space=VMEM)] * 4,
        out_specs=[pl.BlockSpec(memory_space=VMEM)] * 2,
        compiler_params=pltpu.CompilerParams(vmem_limit_bytes=4 * MIB),
        name="finish",
    )(sums, rhs, first, second)


def exchange(pieces, axes):
    return lax.all_to_all(pieces, axes, split_axis=0, concat_axis=0, tiled=True)


def local(
    covariates, lengthscale, nugget, patch_values, patch_weights, block_index, slot_count, owner
):
    devices = lax.axis_size(ALL)
    held, members, cells = patch_values.shape
    slots = patch_weights.shape[1]
    stations = nugget.shape[0]
    capacity = max(2, 2 * held // devices)

    message, z, nugget = terms_of(
        (
            patch_values.reshape(held * members, cells),
            patch_weights.reshape(held * slots, cells),
            block_index.T,
            slot_count[None, :],
            owner.T,
            covariates,
            lengthscale[None, :],
            nugget[None, :],
        ),
        devices,
        capacity,
    )
    own = z[None]
    row_near = [own] + ring(own, COL[0])
    row_joined = jnp.concatenate(row_near)
    column_near = [own] + ring(own, ROW[1])
    column_joined = jnp.concatenate(column_near)
    row_far = ring(row_joined, COL[1])
    column_far = ring(column_joined, ROW[0])
    fi, fj = place(row_near + row_far, column_near + column_far)
    message = exchange(message, ALL)
    rhs, copies = gather_terms(message, (members, stations), lax.axis_size(ROW), capacity, slots)
    gathered = exchange(copies, ROW)
    high, low, partial_value = build_and_product(gathered, fi, fj)
    shares = exchange(partial_value, COL)
    first, copies = total_of(shares, rhs, nugget, lax.axis_size(ROW))
    shares = exchange(kernel_product(exchange(copies, ROW), high, low), COL)
    second, sums = close(shares, rhs, first, nugget)
    copies = jnp.broadcast_to(sums[None], (devices,) + sums.shape)
    sums = exchange(copies, ALL).reshape(devices, sums.shape[1])
    return finish(sums, rhs, first, second)


def solution(mesh):
    torus = Mesh(mesh.devices.reshape(4, 2, 4, 4), ALL)
    placed = (
        P(None, ALL),
        P(),
        P(ALL),
        P(ALL, None, None),
        P(ALL, None, None),
        P(ALL, None),
        P(ALL),
        P(ALL, None),
    )
    return jax.shard_map(
        local,
        mesh=torus,
        in_specs=placed,
        out_specs=(P(None, ALL), P(None, ALL)),
        check_vma=False,
    )
```

```python
import functools
import math

import jax
import jax.numpy as jnp
from jax import lax
from jax.experimental import pallas as pl
from jax.experimental.pallas import tpu as pltpu
from jax.sharding import Mesh
from jax.sharding import PartitionSpec as P

ALL = ("row_0", "row_1", "col_0", "col_1")
COL = ("col_0", "col_1")
ROW = ("row_0", "row_1")

LN2 = math.log(2.0)
SCALE = math.sqrt(5.0) / LN2
FACTOR = LN2 * LN2 / 3.0
LINEAR = 3.0 / LN2
CONST = 3.0 / (LN2 * LN2)
TINY = 1e-30
EARLY, TALL, WIDE = 256, 896, 256
EARLY_COPIES = 4
VALUE_COPIES = 4
VMEM = pltpu.MemorySpace.VMEM
HBM = pltpu.MemorySpace.HBM
MIB = 1 << 20


def rotate(x, axis, by):
    size = lax.axis_size(axis)
    return lax.ppermute(x, axis, [(i, (i + by) % size) for i in range(size)])


def ring(x, axis):
    return [rotate(x, axis, by) for by in range(1, lax.axis_size(axis))]


def halves(x):
    high = x.astype(jnp.bfloat16).astype(jnp.float32)
    return high, x - high


def thirds(x):
    high, rest = halves(x)
    middle, low = halves(rest)
    return high, middle, low


def features(z, left):
    high, middle, low = thirds(z)
    norm = jnp.sum(z * z, axis=0, keepdims=True)
    n_high, n_middle, n_low = thirds(norm)
    row = lax.broadcasted_iota(jnp.int32, z.shape, 0)
    base = 0 if left else 3
    rest = jnp.zeros_like(z)
    for at, part in ((base, n_high), (base + 1, n_middle), (base + 2, n_low)):
        rest = jnp.where(row == at, jnp.broadcast_to(part, z.shape), rest)
    rest = jnp.where((row >= 3 - base) & (row < 6 - base), 1.0, rest)
    if left:
        parts = [high, high, high, middle, middle, low]
    else:
        parts = [-2.0 * part for part in (high, middle, low, high, middle, high)]
    return jnp.concatenate(parts + [rest, jnp.zeros_like(z)], axis=0)


def value_of(squared):
    squared = jnp.maximum(squared, TINY)
    root = squared * lax.rsqrt(squared)
    return (squared + (LINEAR * root + CONST)) * jnp.exp2(-root)


def split_vector(v_ref, vv_ref):
    width = v_ref.shape[2]
    members = vv_ref.shape[0] // 2
    for r in range(v_ref.shape[0]):
        high, low = halves(v_ref[r])
        columns = slice(r * width, (r + 1) * width)
        vv_ref[:members, columns] = high.astype(jnp.bfloat16)
        vv_ref[members:, columns] = low.astype(jnp.bfloat16)


def split_value(squared):
    value = value_of(squared)
    high = value.astype(jnp.bfloat16)
    return high, (value - high.astype(jnp.float32)).astype(jnp.bfloat16)


def early_body(fi_ref, fj_ref, high_out_ref, low_out_ref, high_ref, low_ref, sems):
    tall, columns = high_ref.shape
    last = slice(fj_ref.shape[0] - tall, fj_ref.shape[0])
    chunk = columns // EARLY_COPIES
    copies = []
    for part in range(EARLY_COPIES):
        for tile in range(chunk // WIDE):
            at = slice(part * chunk + tile * WIDE, part * chunk + (tile + 1) * WIDE)
            squared = jnp.dot(
                fj_ref[last, :], fi_ref[:, at], preferred_element_type=jnp.float32
            )
            high_ref[:, at], low_ref[:, at] = split_value(squared)
        at = slice(part * chunk, (part + 1) * chunk)
        for n, (source, target) in enumerate(((high_ref, high_out_ref), (low_ref, low_out_ref))):
            copy = pltpu.make_async_copy(source.at[:, at], target.at[:, at], sems.at[2 * part + n])
            copy.start()
            copies.append(copy)
    for copy in copies:
        copy.wait()


def build_early(fi, fj):
    shape = (EARLY, fi.shape[1])
    return pl.pallas_call(
        early_body,
        out_shape=[HBM(shape, jnp.bfloat16)] * 2,
        in_specs=[pl.BlockSpec(memory_space=VMEM)] * 2,
        out_specs=[pl.BlockSpec(memory_space=HBM)] * 2,
        scratch_shapes=[pltpu.VMEM(shape, jnp.bfloat16)] * 2
        + [pltpu.SemaphoreType.DMA((2 * EARLY_COPIES,))],
        compiler_params=pltpu.CompilerParams(vmem_limit_bytes=20 * MIB),
        cost_estimate=pl.CostEstimate(flops=10**9, bytes_accessed=10**6, transcendentals=0),
        name="early",
    )(fi, fj)


def build_body(
    v_ref,
    fi_ref,
    fj_ref,
    high_in_ref,
    low_in_ref,
    high_ref,
    low_ref,
    out_ref,
    vv_ref,
    acc_ref,
    ahead_ref,
    sems,
):
    members, width = out_ref.shape[1:]
    tall, wide = TALL, WIDE
    tiles, steps = fi_ref.shape[1] // wide, (fj_ref.shape[0] - EARLY) // tall
    last = slice(fj_ref.shape[0] - EARLY, fj_ref.shape[0])
    copies = [
        pltpu.make_async_copy(source, target.at[last, :], sems.at[n])
        for n, (source, target) in enumerate(((high_in_ref, high_ref), (low_in_ref, low_ref)))
    ]
    for copy in copies:
        copy.start()
    split_vector(v_ref, vv_ref)
    acc_ref[...] = jnp.zeros_like(acc_ref)

    def place(step, tile):
        rows = pl.ds(pl.multiple_of(step * tall, tall), tall)
        return rows, slice(tile * wide, (tile + 1) * wide)

    def squares(step, tile):
        rows, columns = place(step, tile)
        return jnp.dot(fj_ref[rows, :], fi_ref[:, columns], preferred_element_type=jnp.float32)

    def product(vv, high, low):
        return jnp.dot(vv, high, preferred_element_type=jnp.float32) + jnp.dot(
            vv, low, preferred_element_type=jnp.float32
        )

    ahead_ref[...] = squares(0, 0)

    @pl.loop(0, steps)
    def _(step):
        squared = ahead_ref[...]
        for tile in range(tiles):
            if tile + 1 < tiles:
                ahead = squares(step, tile + 1)
            else:
                ahead = squares(jnp.minimum(step + 1, steps - 1), 0)
            rows, columns = place(step, tile)
            high, low = split_value(squared)
            high_ref[rows, columns] = high
            low_ref[rows, columns] = low
            acc_ref[:, columns] += product(vv_ref[:, rows], high, low)
            squared = ahead
        ahead_ref[...] = squared

    for copy in copies:
        copy.wait()
    acc = acc_ref[...] + product(vv_ref[:, last], high_ref[last, :], low_ref[last, :])
    total = FACTOR * (acc[:members] + acc[members:])
    for c in range(out_ref.shape[0]):
        out_ref[c] = total[:, c * width : (c + 1) * width]


def build_and_product(v, fi, fj, high, low):
    members, width = v.shape[1:]
    rows, columns = fj.shape[0], fi.shape[1]
    return pl.pallas_call(
        build_body,
        out_shape=[pltpu.VMEM((rows, columns), jnp.bfloat16)] * 2
        + [jax.ShapeDtypeStruct((columns // width, members, width), jnp.float32)],
        in_specs=[pl.BlockSpec(memory_space=VMEM)] * 3 + [pl.BlockSpec(memory_space=HBM)] * 2,
        out_specs=[pl.BlockSpec(memory_space=VMEM)] * 3,
        scratch_shapes=[
            pltpu.VMEM((2 * members, rows), jnp.bfloat16),
            pltpu.VMEM((2 * members, columns), jnp.float32),
            pltpu.VMEM((TALL, WIDE), jnp.float32),
            pltpu.SemaphoreType.DMA((2,)),
        ],
        compiler_params=pltpu.CompilerParams(vmem_limit_bytes=12 * MIB),
        cost_estimate=pl.CostEstimate(
            flops=40 * rows * columns, bytes_accessed=4 * rows * columns, transcendentals=0
        ),
        name="build",
    )(v, fi, fj, *(pltpu.with_memory_space_constraint(x, HBM) for x in (high, low)))


def product_body(v_ref, high_ref, low_ref, out_ref, vv_ref):
    _, members, width = v_ref.shape
    split_vector(v_ref, vv_ref)
    vv = vv_ref[...]
    both = jnp.dot(vv, high_ref[...], preferred_element_type=jnp.float32)
    both += jnp.dot(vv, low_ref[...], preferred_element_type=jnp.float32)
    total = FACTOR * (both[:members] + both[members:])
    for c in range(out_ref.shape[0]):
        out_ref[c] = total[:, c * width : (c + 1) * width]


def kernel_product(v, high, low):
    _, members, width = v.shape
    rows, columns = high.shape
    return pl.pallas_call(
        product_body,
        out_shape=jax.ShapeDtypeStruct((columns // width, members, width), jnp.float32),
        in_specs=[pl.BlockSpec(memory_space=VMEM)] * 3,
        out_specs=pl.BlockSpec(memory_space=VMEM),
        scratch_shapes=[pltpu.VMEM((2 * members, rows), jnp.bfloat16)],
        compiler_params=pltpu.CompilerParams(vmem_limit_bytes=12 * MIB),
        cost_estimate=pl.CostEstimate(
            flops=128 * rows * columns, bytes_accessed=4 * rows * columns, transcendentals=0
        ),
        name="product",
    )(v, high, low)


def to_column(row, size):
    shape = (size, row.shape[1])
    same = lax.broadcasted_iota(jnp.int32, shape, 0) == lax.broadcasted_iota(jnp.int32, shape, 1)
    return jnp.sum(jnp.where(same, jnp.broadcast_to(row, shape), 0.0), axis=1, keepdims=True)


def terms_body(capacity, *refs):
    sources, (out_ref, z_ref, nugget_out_ref) = refs[:8], refs[8:11]
    t_ref, held_refs, sems = refs[11], refs[12:20], refs[20]
    chunk = sources[0].shape[0] // VALUE_COPIES
    parts = [slice(i * chunk, (i + 1) * chunk) for i in range(VALUE_COPIES)]
    pairs = [(sources[0].at[part], held_refs[0].at[part]) for part in parts]
    pairs = list(zip(sources[1:], held_refs[1:])) + pairs
    copies = [pltpu.make_async_copy(*pair, sems.at[i]) for i, pair in enumerate(pairs)]
    for copy in copies[1:7] + copies[:1] + copies[7:]:
        copy.start()
    values_ref, weights_ref, index_ref, count_ref, owner_ref, cov_ref, scale_ref, nugget_ref = held_refs
    slots, held = index_ref.shape
    members = values_ref.shape[0] // held
    lanes = slots * members
    group = 2 * slots

    for copy in copies[1:7]:
        copy.wait()
    z_ref[...] = cov_ref[...] / to_column(scale_ref[...], cov_ref.shape[0])
    nugget_out_ref[...] = nugget_ref[...]
    owner = owner_ref[...].astype(jnp.float32)
    square = (held, held)
    before = lax.broadcasted_iota(jnp.int32, square, 0) < lax.broadcasted_iota(jnp.int32, square, 1)
    shared = (to_column(owner, held) == owner) & before
    rank = jnp.sum(jnp.where(shared, 1.0, 0.0), axis=0, keepdims=True)
    devices = out_ref.shape[0]
    device = lax.broadcasted_iota(jnp.int32, (devices, held), 0).astype(jnp.float32)
    mine = jnp.where(device == owner, 1.0, 0.0)
    count = to_column(count_ref[...].astype(jnp.float32), held)
    index = index_ref[...].astype(jnp.float32)
    ranked = [jnp.where(rank == k, 1.0, 0.0) for k in range(capacity)]
    indices = [index * r for r in ranked]
    indices.append(jnp.zeros((lanes - capacity * slots, held), jnp.float32))
    out_ref[:, 0, capacity * lanes :] = lax.dot_general(
        mine.astype(jnp.bfloat16),
        jnp.concatenate(indices, axis=0).astype(jnp.bfloat16),
        (((1,), (1,)), ((), ())),
        preferred_element_type=jnp.float32,
    )

    copies[0].wait()
    lane = lax.broadcasted_iota(jnp.int32, (slots, lanes), 1)
    own = lane // members == lax.broadcasted_iota(jnp.int32, (slots, lanes), 0)
    for g in range(held // group):
        if g * group * members % chunk == 0:
            copies[7 + g * group * members // chunk].wait()
        weights = weights_ref[g * group * slots : (g + 1) * group * slots, :]
        values = values_ref[g * group * members : (g + 1) * group * members, :]
        every = lax.dot_general(
            weights, values, (((1,), (1,)), ((), ())), preferred_element_type=jnp.float32
        )
        rows = []
        for p in range(group):
            part = every[p * slots : (p + 1) * slots, p // slots * lanes : (p // slots + 1) * lanes]
            turn = (-(p % slots) * members) % lanes
            part = pltpu.roll(part, turn, 1) if turn else part
            part = pltpu.roll(part, 0, 1, stride=members, stride_axis=0)
            rows.append(jnp.sum(jnp.where(own, part, 0.0), axis=0, keepdims=True))
        t_ref[g * group : (g + 1) * group, :] = jnp.concatenate(rows, axis=0)
    slot = (lax.broadcasted_iota(jnp.int32, (held, lanes), 1) // members).astype(jnp.float32)
    terms = jnp.where(slot < count, t_ref[...], 0.0)
    payload = jnp.concatenate(thirds(terms), axis=1).astype(jnp.bfloat16)
    for k in range(capacity):
        table = (mine * ranked[k]).astype(jnp.bfloat16)
        placed = jnp.dot(table, payload, preferred_element_type=jnp.float32)
        out_ref[:, 0, k * lanes : (k + 1) * lanes] = (
            placed[:, :lanes] + placed[:, lanes : 2 * lanes]
        ) + placed[:, 2 * lanes :]


def terms_of(args, devices, capacity):
    values, _, index, _, _, covariates, _, nugget = args
    slots, held = index.shape
    lanes = slots * (values.shape[0] // held)
    return pl.pallas_call(
        functools.partial(terms_body, capacity),
        out_shape=[
            jax.ShapeDtypeStruct((devices, 1, (capacity + 1) * lanes), jnp.float32),
            jax.ShapeDtypeStruct(covariates.shape, jnp.float32),
            jax.ShapeDtypeStruct(nugget.shape, jnp.float32),
        ],
        in_specs=[pl.BlockSpec(memory_space=HBM)] * len(args),
        out_specs=[pl.BlockSpec(memory_space=VMEM)] * 3,
        scratch_shapes=[pltpu.VMEM((held, lanes), jnp.float32)]
        + [pltpu.VMEM(x.shape, x.dtype) for x in args]
        + [pltpu.SemaphoreType.DMA((len(args) - 1 + VALUE_COPIES,))],
        compiler_params=pltpu.CompilerParams(vmem_limit_bytes=8 * MIB),
        cost_estimate=pl.CostEstimate(flops=10**9, bytes_accessed=10**6, transcendentals=0),
        name="terms",
    )(*(pltpu.with_memory_space_constraint(x, HBM) for x in args))


def sources(axes, order):
    outer, inner = (lax.axis_index(name) for name in axes)
    sides = [lax.axis_size(name) for name in axes]
    for by_outer, by_inner in order:
        source = (outer - by_outer + sides[0]) % sides[0] * sides[1]
        yield source + (inner - by_inner + sides[1]) % sides[1]


def place_body(count, *refs):
    pieces, (fi_ref, fj_ref) = refs[:-2], refs[-2:]
    width = pieces[0].shape[2]
    blocks = [(ref, n) for ref in pieces[:count] for n in range(ref.shape[0])]
    sides = [lax.axis_size(name) for name in COL]
    order = [(at % sides[0], at // sides[0]) for at in range(len(blocks))]
    for (ref, n), source in zip(blocks, sources(COL, order)):
        columns = pl.ds(pl.multiple_of(source * width, width), width)
        fi_ref[:, columns] = features(ref[n] * SCALE, False).astype(jnp.bfloat16)
    blocks = [(ref, n) for ref in pieces[count:] for n in range(ref.shape[0])]
    sides = [lax.axis_size(name) for name in ROW]
    order = [(at // sides[1], at % sides[1]) for at in range(len(blocks))]
    for (ref, n), source in zip(blocks, sources(ROW, order)):
        rows = pl.ds(pl.multiple_of(source * width, width), width)
        block = features(ref[n] * SCALE, True)
        fj_ref[rows, :] = jnp.transpose(block.astype(jnp.bfloat16))


def place(row_pieces, column_pieces):
    width = row_pieces[0].shape[2]
    rows = sum(piece.shape[0] for piece in row_pieces) * width
    columns = sum(piece.shape[0] for piece in column_pieces) * width
    return pl.pallas_call(
        functools.partial(place_body, len(row_pieces)),
        out_shape=[
            jax.ShapeDtypeStruct((128, rows), jnp.bfloat16),
            jax.ShapeDtypeStruct((columns, 128), jnp.bfloat16),
        ],
        in_specs=[pl.BlockSpec(memory_space=VMEM)] * len(row_pieces + column_pieces),
        out_specs=[pl.BlockSpec(memory_space=VMEM)] * 2,
        compiler_params=pltpu.CompilerParams(vmem_limit_bytes=4 * MIB),
        cost_estimate=pl.CostEstimate(flops=10**9, bytes_accessed=10**6, transcendentals=0),
        name="place",
    )(*row_pieces, *column_pieces)


def gather_body(capacity, slots, message_ref, rhs_ref, copies_ref):
    devices = message_ref.shape[0]
    members, width = rhs_ref.shape
    lanes = slots * members
    index = jnp.transpose(message_ref[:, 0, capacity * lanes :])
    station = lax.broadcasted_iota(jnp.int32, (width, devices), 0).astype(jnp.float32)
    total = jnp.zeros((3 * members, width), jnp.float32)
    for k in range(capacity):
        terms = jnp.transpose(message_ref[:, 0, k * lanes : (k + 1) * lanes])
        split = [part.astype(jnp.bfloat16) for part in thirds(terms)]
        for s in range(slots):
            at = k * slots + s
            here = jnp.where(station == index[at : at + 1, :], 1.0, 0.0).astype(jnp.bfloat16)
            left = jnp.concatenate([p[s * members : (s + 1) * members] for p in split], axis=0)
            total += lax.dot_general(
                left, here, (((1,), (1,)), ((), ())), preferred_element_type=jnp.float32
            )
    rhs = total[:members] + (total[members : 2 * members] + total[2 * members :])
    rhs_ref[...] = rhs
    for r in range(copies_ref.shape[0]):
        copies_ref[r] = rhs


def gather_terms(message, shape, copies, capacity, slots):
    return pl.pallas_call(
        functools.partial(gather_body, capacity, slots),
        out_shape=[
            jax.ShapeDtypeStruct(shape, jnp.float32),
            jax.ShapeDtypeStruct((copies,) + shape, jnp.float32),
        ],
        in_specs=[pl.BlockSpec(memory_space=VMEM)],
        out_specs=[pl.BlockSpec(memory_space=VMEM)] * 2,
        compiler_params=pltpu.CompilerParams(vmem_limit_bytes=8 * MIB),
        cost_estimate=pl.CostEstimate(flops=10**9, bytes_accessed=10**6, transcendentals=0),
        name="gather",
    )(message)


def total_body(shares_ref, v_ref, nugget_ref, out_ref, copies_ref):
    total = nugget_ref[...] * v_ref[...]
    for c in range(shares_ref.shape[0]):
        total += shares_ref[c]
    out_ref[...] = total
    for r in range(copies_ref.shape[0]):
        copies_ref[r] = total


def total_of(shares, v, nugget, copies):
    return pl.pallas_call(
        total_body,
        out_shape=[
            jax.ShapeDtypeStruct(v.shape, jnp.float32),
            jax.ShapeDtypeStruct((copies,) + v.shape, jnp.float32),
        ],
        in_specs=[pl.BlockSpec(memory_space=VMEM)] * 3,
        out_specs=[pl.BlockSpec(memory_space=VMEM)] * 2,
        compiler_params=pltpu.CompilerParams(vmem_limit_bytes=4 * MIB),
        name="total",
    )(shares, v, nugget)


def guess_of(norm, energy):
    usable = energy > 0.5 * norm
    return jnp.where(usable, norm / jnp.where(usable, energy, 1.0), 0.0)


def close_body(shares_ref, rhs_ref, first_ref, nugget_ref, second_ref, sums_ref):
    rhs, first = rhs_ref[...], first_ref[...]
    second = nugget_ref[...] * first
    for c in range(shares_ref.shape[0]):
        second += shares_ref[c]
    second_ref[...] = second

    def dot(a, b):
        return jnp.sum(a * b, axis=1, keepdims=True)

    norm, energy = dot(rhs, rhs), dot(rhs, first)
    guess = guess_of(norm, energy)
    resid = rhs - guess * first
    along = first - guess * second
    sums = [
        norm,
        energy,
        dot(resid, resid),
        dot(resid, first),
        dot(first, first),
        dot(resid, along),
        dot(resid, second) + dot(first, along),
        dot(first, second),
    ]
    members = rhs.shape[0]
    shape = (members, len(sums) * members)
    row = lax.broadcasted_iota(jnp.int32, shape, 0)
    lane = lax.broadcasted_iota(jnp.int32, shape, 1)
    spaced = jnp.zeros(shape, jnp.float32)
    for at, column in enumerate(sums):
        here = lane == row + at * members
        spaced += jnp.where(here, jnp.broadcast_to(column, shape), 0.0)
    sums_ref[...] = jnp.sum(spaced, axis=0, keepdims=True)


def close(shares, rhs, first, nugget):
    members = rhs.shape[0]
    return pl.pallas_call(
        close_body,
        out_shape=[
            jax.ShapeDtypeStruct(rhs.shape, jnp.float32),
            jax.ShapeDtypeStruct((1, 8 * members), jnp.float32),
        ],
        in_specs=[pl.BlockSpec(memory_space=VMEM)] * 4,
        out_specs=[pl.BlockSpec(memory_space=VMEM)] * 2,
        compiler_params=pltpu.CompilerParams(vmem_limit_bytes=4 * MIB),
        name="close",
    )(shares, rhs, first, nugget)


def finish_body(sums_ref, rhs_ref, first_ref, second_ref, solved_ref, residual_ref):
    rhs, first, second = rhs_ref[...], first_ref[...], second_ref[...]
    members = rhs.shape[0]
    norm, energy, rr, rf, ff, ra, rs, fs = (
        sums_ref[:, q * members : (q + 1) * members] for q in range(8)
    )

    def over(x):
        return jnp.sum(x, axis=0, keepdims=True)

    norm0 = over(norm)
    alpha0 = norm0 / over(energy)
    shift = alpha0 - guess_of(norm, energy)
    norm1 = over(rr - shift * (2.0 * rf - shift * ff))
    energy1 = over(ra - shift * (rs - shift * fs))
    ratio = norm1 / norm0
    alpha1 = norm1 / (energy1 - ratio * norm1 / alpha0)
    shape = (members, members)
    same = lax.broadcasted_iota(jnp.int32, shape, 0) == lax.broadcasted_iota(jnp.int32, shape, 1)

    def column(x):
        return jnp.sum(jnp.where(same, jnp.broadcast_to(x, shape), 0.0), axis=1, keepdims=True)

    alpha0, alpha1, ratio = column(alpha0), column(alpha1), column(ratio)
    residual = rhs - alpha0 * first
    direction = residual + ratio * rhs
    along = (first - alpha0 * second) + ratio * first
    solved_ref[...] = alpha0 * rhs + alpha1 * direction
    residual_ref[...] = residual - alpha1 * along


def finish(sums, rhs, first, second):
    return pl.pallas_call(
        finish_body,
        out_shape=[jax.ShapeDtypeStruct(rhs.shape, jnp.float32)] * 2,
        in_specs=[pl.BlockSpec(memory_space=VMEM)] * 4,
        out_specs=[pl.BlockSpec(memory_space=VMEM)] * 2,
        compiler_params=pltpu.CompilerParams(vmem_limit_bytes=4 * MIB),
        name="finish",
    )(sums, rhs, first, second)


def exchange(pieces, axes):
    return lax.all_to_all(pieces, axes, split_axis=0, concat_axis=0, tiled=True)


def local(
    covariates, lengthscale, nugget, patch_values, patch_weights, block_index, slot_count, owner
):
    devices = lax.axis_size(ALL)
    held, members, cells = patch_values.shape
    slots = patch_weights.shape[1]
    stations = nugget.shape[0]
    capacity = max(2, 2 * held // devices)

    message, z, nugget = terms_of(
        (
            patch_values.reshape(held * members, cells),
            patch_weights.reshape(held * slots, cells),
            block_index.T,
            slot_count[None, :],
            owner.T,
            covariates,
            lengthscale[None, :],
            nugget[None, :],
        ),
        devices,
        capacity,
    )
    own = z[None]
    row_near = [own] + ring(own, COL[0])
    row_joined = jnp.concatenate(row_near)
    column_near = [own] + ring(own, ROW[1])
    column_joined = jnp.concatenate(column_near)
    row_far = ring(row_joined, COL[1])
    column_far = ring(column_joined, ROW[0])
    fi, fj = place(row_near + row_far, column_near + column_far)
    high, low = build_early(fi, fj)
    message = exchange(message, ALL)
    rhs, copies = gather_terms(message, (members, stations), lax.axis_size(ROW), capacity, slots)
    gathered = exchange(copies, ROW)
    high, low, partial_value = build_and_product(gathered, fi, fj, high, low)
    shares = exchange(partial_value, COL)
    first, copies = total_of(shares, rhs, nugget, lax.axis_size(ROW))
    shares = exchange(kernel_product(exchange(copies, ROW), high, low), COL)
    second, sums = close(shares, rhs, first, nugget)
    copies = jnp.broadcast_to(sums[None], (devices,) + sums.shape)
    sums = exchange(copies, ALL).reshape(devices, sums.shape[1])
    return finish(sums, rhs, first, second)


def solution(mesh):
    torus = Mesh(mesh.devices.reshape(4, 2, 4, 4), ALL)
    placed = (
        P(None, ALL),
        P(),
        P(ALL),
        P(ALL, None, None),
        P(ALL, None, None),
        P(ALL, None),
        P(ALL),
        P(ALL, None),
    )
    return jax.shard_map(
        local,
        mesh=torus,
        in_specs=placed,
        out_specs=(P(None, ALL), P(None, ALL)),
        check_vma=False,
    )
```

```python
import functools
import math

import jax
import jax.numpy as jnp
from jax import lax
from jax.experimental import pallas as pl
from jax.experimental.pallas import tpu as pltpu
from jax.sharding import Mesh
from jax.sharding import PartitionSpec as P

ALL = ("row_0", "row_1", "col_0", "col_1")
COL = ("col_0", "col_1")
ROW = ("row_0", "row_1")

LN2 = math.log(2.0)
SCALE = math.sqrt(5.0) / LN2
FACTOR = LN2 * LN2 / 3.0
LINEAR = 3.0 / LN2
CONST = 3.0 / (LN2 * LN2)
TINY = 1e-30
EARLY, TALL, WIDE = 256, 896, 256
EARLY_COPIES = 4
VALUE_COPIES = 4
VMEM = pltpu.MemorySpace.VMEM
HBM = pltpu.MemorySpace.HBM
MIB = 1 << 20


def rotate(x, axis, by):
    size = lax.axis_size(axis)
    return lax.ppermute(x, axis, [(i, (i + by) % size) for i in range(size)])


def ring(x, axis):
    return [rotate(x, axis, by) for by in range(1, lax.axis_size(axis))]


def halves(x):
    high = x.astype(jnp.bfloat16).astype(jnp.float32)
    return high, x - high


def thirds(x):
    high, rest = halves(x)
    middle, low = halves(rest)
    return high, middle, low


def features(z, left):
    high, middle, low = thirds(z)
    norm = jnp.sum(z * z, axis=0, keepdims=True)
    n_high, n_middle, n_low = thirds(norm)
    row = lax.broadcasted_iota(jnp.int32, z.shape, 0)
    base = 0 if left else 3
    rest = jnp.zeros_like(z)
    for at, part in ((base, n_high), (base + 1, n_middle), (base + 2, n_low)):
        rest = jnp.where(row == at, jnp.broadcast_to(part, z.shape), rest)
    rest = jnp.where((row >= 3 - base) & (row < 6 - base), 1.0, rest)
    if left:
        parts = [high, high, high, middle, middle, low]
    else:
        parts = [-2.0 * part for part in (high, middle, low, high, middle, high)]
    return jnp.concatenate(parts + [rest, jnp.zeros_like(z)], axis=0)


def value_of(squared):
    squared = jnp.maximum(squared, TINY)
    root = squared * lax.rsqrt(squared)
    return (squared + (LINEAR * root + CONST)) * jnp.exp2(-root)


def split_vector(v_ref, vv_ref):
    width = v_ref.shape[2]
    members = vv_ref.shape[0] // 2
    for r in range(v_ref.shape[0]):
        high, low = halves(v_ref[r])
        columns = slice(r * width, (r + 1) * width)
        vv_ref[:members, columns] = high.astype(jnp.bfloat16)
        vv_ref[members:, columns] = low.astype(jnp.bfloat16)


def split_value(value):
    high = value.astype(jnp.bfloat16)
    return high, (value - high.astype(jnp.float32)).astype(jnp.bfloat16)


def half_of(sides, columns):
    half = sides[0].shape[1]
    at = columns.start // half
    return sides[at], slice(columns.start - at * half, columns.stop - at * half)


def product(vv, value):
    high, low = split_value(value)
    return jnp.dot(vv, high, preferred_element_type=jnp.float32) + jnp.dot(
        vv, low, preferred_element_type=jnp.float32
    )


def early_body(fi_ref, fj_ref, sent_ref, value_ref, sems):
    tall, columns = value_ref.shape
    last = slice(fj_ref.shape[0] - tall, fj_ref.shape[0])
    chunk = columns // EARLY_COPIES
    copies = []
    for part in range(EARLY_COPIES):
        for tile in range(chunk // WIDE):
            at = slice(part * chunk + tile * WIDE, part * chunk + (tile + 1) * WIDE)
            squared = jnp.dot(
                fj_ref[last, :], fi_ref[:, at], preferred_element_type=jnp.float32
            )
            value_ref[:, at] = value_of(squared)
        at = slice(part * chunk, (part + 1) * chunk)
        copies.append(
            pltpu.make_async_copy(value_ref.at[:, at], sent_ref.at[:, at], sems.at[part])
        )
        copies[-1].start()
    for copy in copies:
        copy.wait()


def build_early(fi, fj):
    shape = (EARLY, fi.shape[1])
    return pl.pallas_call(
        early_body,
        out_shape=HBM(shape, jnp.float32),
        in_specs=[pl.BlockSpec(memory_space=VMEM)] * 2,
        out_specs=pl.BlockSpec(memory_space=HBM),
        scratch_shapes=[
            pltpu.VMEM(shape, jnp.float32),
            pltpu.SemaphoreType.DMA((EARLY_COPIES,)),
        ],
        compiler_params=pltpu.CompilerParams(vmem_limit_bytes=20 * MIB),
        cost_estimate=pl.CostEstimate(flops=10**9, bytes_accessed=10**6, transcendentals=0),
        name="early",
    )(fi, fj)


def build_body(
    v_ref,
    fi_ref,
    fj_ref,
    early_ref,
    left_ref,
    right_ref,
    out_ref,
    vv_ref,
    acc_ref,
    ahead_ref,
    sems,
):
    members, width = out_ref.shape[1:]
    tall, wide = TALL, WIDE
    tiles, steps = fi_ref.shape[1] // wide, (fj_ref.shape[0] - EARLY) // tall
    last = slice(fj_ref.shape[0] - EARLY, fj_ref.shape[0])
    half = left_ref.shape[1]
    copies = [
        pltpu.make_async_copy(early_ref.at[:, :half], left_ref.at[last, :], sems.at[0]),
        pltpu.make_async_copy(early_ref.at[:, half:], right_ref.at[last, :], sems.at[1]),
    ]
    for copy in copies:
        copy.start()
    split_vector(v_ref, vv_ref)
    acc_ref[...] = jnp.zeros_like(acc_ref)

    def place(step, tile):
        rows = pl.ds(pl.multiple_of(step * tall, tall), tall)
        return rows, slice(tile * wide, (tile + 1) * wide)

    def squares(step, tile):
        rows, columns = place(step, tile)
        return jnp.dot(fj_ref[rows, :], fi_ref[:, columns], preferred_element_type=jnp.float32)

    ahead_ref[...] = squares(0, 0)

    @pl.loop(0, steps)
    def _(step):
        squared = ahead_ref[...]
        for tile in range(tiles):
            if tile + 1 < tiles:
                ahead = squares(step, tile + 1)
            else:
                ahead = squares(jnp.minimum(step + 1, steps - 1), 0)
            rows, columns = place(step, tile)
            value = value_of(squared)
            side, within = half_of((left_ref, right_ref), columns)
            side[rows, within] = value
            acc_ref[:, columns] += product(vv_ref[:, rows], value)
            squared = ahead
        ahead_ref[...] = squared

    for copy in copies:
        copy.wait()
    for c in range(out_ref.shape[0]):
        columns = slice(c * width, (c + 1) * width)
        side, within = half_of((left_ref, right_ref), columns)
        acc = acc_ref[:, columns] + product(vv_ref[:, last], side[last, within])
        out_ref[c] = FACTOR * (acc[:members] + acc[members:])


def build_and_product(v, fi, fj, early):
    members, width = v.shape[1:]
    rows, columns = fj.shape[0], fi.shape[1]
    return pl.pallas_call(
        build_body,
        out_shape=[
            pltpu.VMEM((rows, columns // 2), jnp.float32),
            pltpu.VMEM((rows, columns // 2), jnp.float32),
            jax.ShapeDtypeStruct((columns // width, members, width), jnp.float32),
        ],
        in_specs=[pl.BlockSpec(memory_space=VMEM)] * 3 + [pl.BlockSpec(memory_space=HBM)],
        out_specs=[pl.BlockSpec(memory_space=VMEM)] * 3,
        scratch_shapes=[
            pltpu.VMEM((2 * members, rows), jnp.bfloat16),
            pltpu.VMEM((2 * members, columns), jnp.float32),
            pltpu.VMEM((TALL, WIDE), jnp.float32),
            pltpu.SemaphoreType.DMA((2,)),
        ],
        compiler_params=pltpu.CompilerParams(vmem_limit_bytes=12 * MIB),
        cost_estimate=pl.CostEstimate(
            flops=40 * rows * columns, bytes_accessed=4 * rows * columns, transcendentals=0
        ),
        name="build",
    )(v, fi, fj, pltpu.with_memory_space_constraint(early, HBM))


def product_body(v_ref, left_ref, right_ref, out_ref, vv_ref):
    count, members, width = v_ref.shape
    split_vector(v_ref, vv_ref)
    for c in range(out_ref.shape[0]):
        columns = slice(c * width, (c + 1) * width)
        side, within = half_of((left_ref, right_ref), columns)
        acc = jnp.zeros((2 * members, width), jnp.float32)
        for r in range(count):
            rows = slice(r * width, (r + 1) * width)
            acc += product(vv_ref[:, rows], side[rows, within])
        out_ref[c] = FACTOR * (acc[:members] + acc[members:])


def kernel_product(v, left, right):
    _, members, width = v.shape
    rows, columns = left.shape[0], 2 * left.shape[1]
    return pl.pallas_call(
        product_body,
        out_shape=jax.ShapeDtypeStruct((columns // width, members, width), jnp.float32),
        in_specs=[pl.BlockSpec(memory_space=VMEM)] * 3,
        out_specs=pl.BlockSpec(memory_space=VMEM),
        scratch_shapes=[pltpu.VMEM((2 * members, rows), jnp.bfloat16)],
        compiler_params=pltpu.CompilerParams(vmem_limit_bytes=12 * MIB),
        cost_estimate=pl.CostEstimate(
            flops=128 * rows * columns, bytes_accessed=4 * rows * columns, transcendentals=0
        ),
        name="product",
    )(v, left, right)


def to_column(row, size):
    shape = (size, row.shape[1])
    same = lax.broadcasted_iota(jnp.int32, shape, 0) == lax.broadcasted_iota(jnp.int32, shape, 1)
    return jnp.sum(jnp.where(same, jnp.broadcast_to(row, shape), 0.0), axis=1, keepdims=True)


def terms_body(capacity, *refs):
    sources, (out_ref, z_ref, nugget_out_ref) = refs[:8], refs[8:11]
    t_ref, held_refs, sems = refs[11], refs[12:20], refs[20]
    chunk = sources[0].shape[0] // VALUE_COPIES
    parts = [slice(i * chunk, (i + 1) * chunk) for i in range(VALUE_COPIES)]
    pairs = [(sources[0].at[part], held_refs[0].at[part]) for part in parts]
    pairs = list(zip(sources[1:], held_refs[1:])) + pairs
    copies = [pltpu.make_async_copy(*pair, sems.at[i]) for i, pair in enumerate(pairs)]
    for copy in copies[1:7] + copies[:1] + copies[7:]:
        copy.start()
    values_ref, weights_ref, index_ref, count_ref, owner_ref, cov_ref, scale_ref, nugget_ref = held_refs
    slots, held = index_ref.shape
    members = values_ref.shape[0] // held
    lanes = slots * members
    group = 2 * slots

    for copy in copies[1:7]:
        copy.wait()
    z_ref[...] = cov_ref[...] / to_column(scale_ref[...], cov_ref.shape[0])
    nugget_out_ref[...] = nugget_ref[...]
    owner = owner_ref[...].astype(jnp.float32)
    square = (held, held)
    before = lax.broadcasted_iota(jnp.int32, square, 0) < lax.broadcasted_iota(jnp.int32, square, 1)
    shared = (to_column(owner, held) == owner) & before
    rank = jnp.sum(jnp.where(shared, 1.0, 0.0), axis=0, keepdims=True)
    devices = out_ref.shape[0]
    device = lax.broadcasted_iota(jnp.int32, (devices, held), 0).astype(jnp.float32)
    mine = jnp.where(device == owner, 1.0, 0.0)
    count = to_column(count_ref[...].astype(jnp.float32), held)
    index = index_ref[...].astype(jnp.float32)
    ranked = [jnp.where(rank == k, 1.0, 0.0) for k in range(capacity)]
    indices = [index * r for r in ranked]
    indices.append(jnp.zeros((lanes - capacity * slots, held), jnp.float32))
    out_ref[:, 0, capacity * lanes :] = lax.dot_general(
        mine.astype(jnp.bfloat16),
        jnp.concatenate(indices, axis=0).astype(jnp.bfloat16),
        (((1,), (1,)), ((), ())),
        preferred_element_type=jnp.float32,
    )

    copies[0].wait()
    lane = lax.broadcasted_iota(jnp.int32, (slots, lanes), 1)
    own = lane // members == lax.broadcasted_iota(jnp.int32, (slots, lanes), 0)
    for g in range(held // group):
        if g * group * members % chunk == 0:
            copies[7 + g * group * members // chunk].wait()
        weights = weights_ref[g * group * slots : (g + 1) * group * slots, :]
        values = values_ref[g * group * members : (g + 1) * group * members, :]
        every = lax.dot_general(
            weights, values, (((1,), (1,)), ((), ())), preferred_element_type=jnp.float32
        )
        rows = []
        for p in range(group):
            part = every[p * slots : (p + 1) * slots, p // slots * lanes : (p // slots + 1) * lanes]
            turn = (-(p % slots) * members) % lanes
            part = pltpu.roll(part, turn, 1) if turn else part
            part = pltpu.roll(part, 0, 1, stride=members, stride_axis=0)
            rows.append(jnp.sum(jnp.where(own, part, 0.0), axis=0, keepdims=True))
        t_ref[g * group : (g + 1) * group, :] = jnp.concatenate(rows, axis=0)
    slot = (lax.broadcasted_iota(jnp.int32, (held, lanes), 1) // members).astype(jnp.float32)
    terms = jnp.where(slot < count, t_ref[...], 0.0)
    payload = jnp.concatenate(thirds(terms), axis=1).astype(jnp.bfloat16)
    for k in range(capacity):
        table = (mine * ranked[k]).astype(jnp.bfloat16)
        placed = jnp.dot(table, payload, preferred_element_type=jnp.float32)
        out_ref[:, 0, k * lanes : (k + 1) * lanes] = (
            placed[:, :lanes] + placed[:, lanes : 2 * lanes]
        ) + placed[:, 2 * lanes :]


def terms_of(args, devices, capacity):
    values, _, index, _, _, covariates, _, nugget = args
    slots, held = index.shape
    lanes = slots * (values.shape[0] // held)
    return pl.pallas_call(
        functools.partial(terms_body, capacity),
        out_shape=[
            jax.ShapeDtypeStruct((devices, 1, (capacity + 1) * lanes), jnp.float32),
            jax.ShapeDtypeStruct(covariates.shape, jnp.float32),
            jax.ShapeDtypeStruct(nugget.shape, jnp.float32),
        ],
        in_specs=[pl.BlockSpec(memory_space=HBM)] * len(args),
        out_specs=[pl.BlockSpec(memory_space=VMEM)] * 3,
        scratch_shapes=[pltpu.VMEM((held, lanes), jnp.float32)]
        + [pltpu.VMEM(x.shape, x.dtype) for x in args]
        + [pltpu.SemaphoreType.DMA((len(args) - 1 + VALUE_COPIES,))],
        compiler_params=pltpu.CompilerParams(vmem_limit_bytes=8 * MIB),
        cost_estimate=pl.CostEstimate(flops=10**9, bytes_accessed=10**6, transcendentals=0),
        name="terms",
    )(*(pltpu.with_memory_space_constraint(x, HBM) for x in args))


def sources(axes, order):
    outer, inner = (lax.axis_index(name) for name in axes)
    sides = [lax.axis_size(name) for name in axes]
    for by_outer, by_inner in order:
        source = (outer - by_outer + sides[0]) % sides[0] * sides[1]
        yield source + (inner - by_inner + sides[1]) % sides[1]


def place_body(count, *refs):
    pieces, (fi_ref, fj_ref) = refs[:-2], refs[-2:]
    width = pieces[0].shape[2]
    blocks = [(ref, n) for ref in pieces[:count] for n in range(ref.shape[0])]
    sides = [lax.axis_size(name) for name in COL]
    order = [(at % sides[0], at // sides[0]) for at in range(len(blocks))]
    for (ref, n), source in zip(blocks, sources(COL, order)):
        columns = pl.ds(pl.multiple_of(source * width, width), width)
        fi_ref[:, columns] = features(ref[n] * SCALE, False).astype(jnp.bfloat16)
    blocks = [(ref, n) for ref in pieces[count:] for n in range(ref.shape[0])]
    sides = [lax.axis_size(name) for name in ROW]
    order = [(at // sides[1], at % sides[1]) for at in range(len(blocks))]
    for (ref, n), source in zip(blocks, sources(ROW, order)):
        rows = pl.ds(pl.multiple_of(source * width, width), width)
        block = features(ref[n] * SCALE, True)
        fj_ref[rows, :] = jnp.transpose(block.astype(jnp.bfloat16))


def place(row_pieces, column_pieces):
    width = row_pieces[0].shape[2]
    rows = sum(piece.shape[0] for piece in row_pieces) * width
    columns = sum(piece.shape[0] for piece in column_pieces) * width
    return pl.pallas_call(
        functools.partial(place_body, len(row_pieces)),
        out_shape=[
            jax.ShapeDtypeStruct((128, rows), jnp.bfloat16),
            jax.ShapeDtypeStruct((columns, 128), jnp.bfloat16),
        ],
        in_specs=[pl.BlockSpec(memory_space=VMEM)] * len(row_pieces + column_pieces),
        out_specs=[pl.BlockSpec(memory_space=VMEM)] * 2,
        compiler_params=pltpu.CompilerParams(vmem_limit_bytes=4 * MIB),
        cost_estimate=pl.CostEstimate(flops=10**9, bytes_accessed=10**6, transcendentals=0),
        name="place",
    )(*row_pieces, *column_pieces)


def gather_body(capacity, slots, message_ref, rhs_ref, copies_ref):
    devices = message_ref.shape[0]
    members, width = rhs_ref.shape
    lanes = slots * members
    index = jnp.transpose(message_ref[:, 0, capacity * lanes :])
    station = lax.broadcasted_iota(jnp.int32, (width, devices), 0).astype(jnp.float32)
    total = jnp.zeros((3 * members, width), jnp.float32)
    for k in range(capacity):
        terms = jnp.transpose(message_ref[:, 0, k * lanes : (k + 1) * lanes])
        split = [part.astype(jnp.bfloat16) for part in thirds(terms)]
        for s in range(slots):
            at = k * slots + s
            here = jnp.where(station == index[at : at + 1, :], 1.0, 0.0).astype(jnp.bfloat16)
            left = jnp.concatenate([p[s * members : (s + 1) * members] for p in split], axis=0)
            total += lax.dot_general(
                left, here, (((1,), (1,)), ((), ())), preferred_element_type=jnp.float32
            )
    rhs = total[:members] + (total[members : 2 * members] + total[2 * members :])
    rhs_ref[...] = rhs
    for r in range(copies_ref.shape[0]):
        copies_ref[r] = rhs


def gather_terms(message, shape, copies, capacity, slots):
    return pl.pallas_call(
        functools.partial(gather_body, capacity, slots),
        out_shape=[
            jax.ShapeDtypeStruct(shape, jnp.float32),
            jax.ShapeDtypeStruct((copies,) + shape, jnp.float32),
        ],
        in_specs=[pl.BlockSpec(memory_space=VMEM)],
        out_specs=[pl.BlockSpec(memory_space=VMEM)] * 2,
        compiler_params=pltpu.CompilerParams(vmem_limit_bytes=8 * MIB),
        cost_estimate=pl.CostEstimate(flops=10**9, bytes_accessed=10**6, transcendentals=0),
        name="gather",
    )(message)


def total_body(shares_ref, v_ref, nugget_ref, out_ref, copies_ref):
    total = nugget_ref[...] * v_ref[...]
    for c in range(shares_ref.shape[0]):
        total += shares_ref[c]
    out_ref[...] = total
    for r in range(copies_ref.shape[0]):
        copies_ref[r] = total


def total_of(shares, v, nugget, copies):
    return pl.pallas_call(
        total_body,
        out_shape=[
            jax.ShapeDtypeStruct(v.shape, jnp.float32),
            jax.ShapeDtypeStruct((copies,) + v.shape, jnp.float32),
        ],
        in_specs=[pl.BlockSpec(memory_space=VMEM)] * 3,
        out_specs=[pl.BlockSpec(memory_space=VMEM)] * 2,
        compiler_params=pltpu.CompilerParams(vmem_limit_bytes=4 * MIB),
        name="total",
    )(shares, v, nugget)


def guess_of(norm, energy):
    usable = energy > 0.5 * norm
    return jnp.where(usable, norm / jnp.where(usable, energy, 1.0), 0.0)


def close_body(shares_ref, rhs_ref, first_ref, nugget_ref, second_ref, sums_ref):
    rhs, first = rhs_ref[...], first_ref[...]
    second = nugget_ref[...] * first
    for c in range(shares_ref.shape[0]):
        second += shares_ref[c]
    second_ref[...] = second

    def dot(a, b):
        return jnp.sum(a * b, axis=1, keepdims=True)

    norm, energy = dot(rhs, rhs), dot(rhs, first)
    guess = guess_of(norm, energy)
    resid = rhs - guess * first
    along = first - guess * second
    sums = [
        norm,
        energy,
        dot(resid, resid),
        dot(resid, first),
        dot(first, first),
        dot(resid, along),
        dot(resid, second) + dot(first, along),
        dot(first, second),
    ]
    members = rhs.shape[0]
    shape = (members, len(sums) * members)
    row = lax.broadcasted_iota(jnp.int32, shape, 0)
    lane = lax.broadcasted_iota(jnp.int32, shape, 1)
    spaced = jnp.zeros(shape, jnp.float32)
    for at, column in enumerate(sums):
        here = lane == row + at * members
        spaced += jnp.where(here, jnp.broadcast_to(column, shape), 0.0)
    sums_ref[...] = jnp.broadcast_to(jnp.sum(spaced, axis=0, keepdims=True), sums_ref.shape)


def close(shares, rhs, first, nugget, devices):
    members = rhs.shape[0]
    return pl.pallas_call(
        close_body,
        out_shape=[
            jax.ShapeDtypeStruct(rhs.shape, jnp.float32),
            jax.ShapeDtypeStruct((devices, 8 * members), jnp.float32),
        ],
        in_specs=[pl.BlockSpec(memory_space=VMEM)] * 4,
        out_specs=[pl.BlockSpec(memory_space=VMEM)] * 2,
        compiler_params=pltpu.CompilerParams(vmem_limit_bytes=4 * MIB),
        name="close",
    )(shares, rhs, first, nugget)


def finish_body(sums_ref, rhs_ref, first_ref, second_ref, solved_ref, residual_ref):
    rhs, first, second = rhs_ref[...], first_ref[...], second_ref[...]
    members = rhs.shape[0]
    norm, energy, rr, rf, ff, ra, rs, fs = (
        sums_ref[:, q * members : (q + 1) * members] for q in range(8)
    )

    def over(x):
        return jnp.sum(x, axis=0, keepdims=True)

    norm0 = over(norm)
    alpha0 = norm0 / over(energy)
    shift = alpha0 - guess_of(norm, energy)
    norm1 = over(rr - shift * (2.0 * rf - shift * ff))
    energy1 = over(ra - shift * (rs - shift * fs))
    ratio = norm1 / norm0
    alpha1 = norm1 / (energy1 - ratio * norm1 / alpha0)
    shape = (members, members)
    same = lax.broadcasted_iota(jnp.int32, shape, 0) == lax.broadcasted_iota(jnp.int32, shape, 1)

    def column(x):
        return jnp.sum(jnp.where(same, jnp.broadcast_to(x, shape), 0.0), axis=1, keepdims=True)

    alpha0, alpha1, ratio = column(alpha0), column(alpha1), column(ratio)
    residual = rhs - alpha0 * first
    direction = residual + ratio * rhs
    along = (first - alpha0 * second) + ratio * first
    solved_ref[...] = alpha0 * rhs + alpha1 * direction
    residual_ref[...] = residual - alpha1 * along


def finish(sums, rhs, first, second):
    return pl.pallas_call(
        finish_body,
        out_shape=[jax.ShapeDtypeStruct(rhs.shape, jnp.float32)] * 2,
        in_specs=[pl.BlockSpec(memory_space=VMEM)] * 4,
        out_specs=[pl.BlockSpec(memory_space=VMEM)] * 2,
        compiler_params=pltpu.CompilerParams(vmem_limit_bytes=4 * MIB),
        name="finish",
    )(sums, rhs, first, second)


def exchange(pieces, axes):
    return lax.all_to_all(pieces, axes, split_axis=0, concat_axis=0, tiled=True)


def local(
    covariates, lengthscale, nugget, patch_values, patch_weights, block_index, slot_count, owner
):
    devices = lax.axis_size(ALL)
    held, members, cells = patch_values.shape
    slots = patch_weights.shape[1]
    stations = nugget.shape[0]
    capacity = max(2, 2 * held // devices)

    message, z, nugget = terms_of(
        (
            patch_values.reshape(held * members, cells),
            patch_weights.reshape(held * slots, cells),
            block_index.T,
            slot_count[None, :],
            owner.T,
            covariates,
            lengthscale[None, :],
            nugget[None, :],
        ),
        devices,
        capacity,
    )
    own = z[None]
    row_near = [own] + ring(own, COL[0])
    row_joined = jnp.concatenate(row_near)
    column_near = [own] + ring(own, ROW[1])
    column_joined = jnp.concatenate(column_near)
    row_far = ring(row_joined, COL[1])
    column_far = ring(column_joined, ROW[0])
    fi, fj = place(row_near + row_far, column_near + column_far)
    early = build_early(fi, fj)
    message = exchange(message, ALL)
    rhs, copies = gather_terms(message, (members, stations), lax.axis_size(ROW), capacity, slots)
    gathered = exchange(copies, ROW)
    left, right, partial_value = build_and_product(gathered, fi, fj, early)
    shares = exchange(partial_value, COL)
    first, copies = total_of(shares, rhs, nugget, lax.axis_size(ROW))
    shares = exchange(kernel_product(exchange(copies, ROW), left, right), COL)
    second, sums = close(shares, rhs, first, nugget, devices)
    sums = exchange(sums[:, None, :], ALL)[:, 0, :]
    return finish(sums, rhs, first, second)


def solution(mesh):
    torus = Mesh(mesh.devices.reshape(4, 2, 4, 4), ALL)
    placed = (
        P(None, ALL),
        P(),
        P(ALL),
        P(ALL, None, None),
        P(ALL, None, None),
        P(ALL, None),
        P(ALL),
        P(ALL, None),
    )
    return jax.shard_map(
        local,
        mesh=torus,
        in_specs=placed,
        out_specs=(P(None, ALL), P(None, ALL)),
        check_vma=False,
    )
```

```python
import functools
import math

import jax
import jax.numpy as jnp
from jax import lax
from jax.experimental import pallas as pl
from jax.experimental.pallas import tpu as pltpu
from jax.sharding import Mesh
from jax.sharding import PartitionSpec as P

ALL = ("row_0", "row_1", "col_0", "col_1")
COL = ("col_0", "col_1")
ROW = ("row_0", "row_1")

LN2 = math.log(2.0)
SCALE = math.sqrt(5.0) / LN2
FACTOR = LN2 * LN2 / 3.0
LINEAR = 3.0 / LN2
CONST = 3.0 / (LN2 * LN2)
TINY = 1e-30
EARLY, TALL, WIDE = 256, 896, 256
EARLY_COPIES = 4
VALUE_COPIES = 4
VMEM = pltpu.MemorySpace.VMEM
HBM = pltpu.MemorySpace.HBM
MIB = 1 << 20


def rotate(x, axis, by):
    size = lax.axis_size(axis)
    return lax.ppermute(x, axis, [(i, (i + by) % size) for i in range(size)])


def ring(x, axis):
    return [rotate(x, axis, by) for by in range(1, lax.axis_size(axis))]


def halves(x):
    high = x.astype(jnp.bfloat16).astype(jnp.float32)
    return high, x - high


def thirds(x):
    high, rest = halves(x)
    middle, low = halves(rest)
    return high, middle, low


def features(z, left):
    high, middle, low = thirds(z)
    norm = jnp.sum(z * z, axis=0, keepdims=True)
    n_high, n_middle, n_low = thirds(norm)
    row = lax.broadcasted_iota(jnp.int32, z.shape, 0)
    base = 0 if left else 3
    rest = jnp.zeros_like(z)
    for at, part in ((base, n_high), (base + 1, n_middle), (base + 2, n_low)):
        rest = jnp.where(row == at, jnp.broadcast_to(part, z.shape), rest)
    rest = jnp.where((row >= 3 - base) & (row < 6 - base), 1.0, rest)
    if left:
        parts = [high, high, high, middle, middle, low]
    else:
        parts = [-2.0 * part for part in (high, middle, low, high, middle, high)]
    return jnp.concatenate(parts + [rest, jnp.zeros_like(z)], axis=0)


def value_of(squared):
    squared = jnp.maximum(squared, TINY)
    root = squared * lax.rsqrt(squared)
    return (squared + (LINEAR * root + CONST)) * jnp.exp2(-root)


def split_vector(v_ref, vv_ref):
    width = v_ref.shape[2]
    members = vv_ref.shape[0] // 2
    for r in range(v_ref.shape[0]):
        high, low = halves(v_ref[r])
        columns = slice(r * width, (r + 1) * width)
        vv_ref[:members, columns] = high.astype(jnp.bfloat16)
        vv_ref[members:, columns] = low.astype(jnp.bfloat16)


def split_value(value):
    high = value.astype(jnp.bfloat16)
    return high, (value - high.astype(jnp.float32)).astype(jnp.bfloat16)


def half_of(sides, columns):
    half = sides[0].shape[1]
    at = columns.start // half
    return sides[at], slice(columns.start - at * half, columns.stop - at * half)


def product(vv, value):
    high, low = split_value(value)
    return jnp.dot(vv, high, preferred_element_type=jnp.float32) + jnp.dot(
        vv, low, preferred_element_type=jnp.float32
    )


def early_body(fi_ref, fj_ref, sent_ref, value_ref, sems):
    tall, columns = value_ref.shape
    last = slice(fj_ref.shape[0] - tall, fj_ref.shape[0])
    chunk = columns // EARLY_COPIES
    copies = []
    for part in range(EARLY_COPIES):
        for tile in range(chunk // WIDE):
            at = slice(part * chunk + tile * WIDE, part * chunk + (tile + 1) * WIDE)
            squared = jnp.dot(
                fj_ref[last, :], fi_ref[:, at], preferred_element_type=jnp.float32
            )
            value_ref[:, at] = value_of(squared)
        at = slice(part * chunk, (part + 1) * chunk)
        copies.append(
            pltpu.make_async_copy(value_ref.at[:, at], sent_ref.at[:, at], sems.at[part])
        )
        copies[-1].start()
    for copy in copies:
        copy.wait()


def build_early(fi, fj):
    shape = (EARLY, fi.shape[1])
    return pl.pallas_call(
        early_body,
        out_shape=HBM(shape, jnp.float32),
        in_specs=[pl.BlockSpec(memory_space=VMEM)] * 2,
        out_specs=pl.BlockSpec(memory_space=HBM),
        scratch_shapes=[
            pltpu.VMEM(shape, jnp.float32),
            pltpu.SemaphoreType.DMA((EARLY_COPIES,)),
        ],
        compiler_params=pltpu.CompilerParams(vmem_limit_bytes=20 * MIB),
        cost_estimate=pl.CostEstimate(flops=10**9, bytes_accessed=10**6, transcendentals=0),
        name="early",
    )(fi, fj)


def build_body(
    v_ref,
    fi_ref,
    fj_ref,
    early_ref,
    left_ref,
    right_ref,
    out_ref,
    vv_ref,
    acc_ref,
    ahead_ref,
    sems,
):
    members, width = out_ref.shape[1:]
    tall, wide = TALL, WIDE
    tiles, steps = fi_ref.shape[1] // wide, (fj_ref.shape[0] - EARLY) // tall
    last = slice(fj_ref.shape[0] - EARLY, fj_ref.shape[0])
    half = left_ref.shape[1]
    copies = [
        pltpu.make_async_copy(early_ref.at[:, :half], left_ref.at[last, :], sems.at[0]),
        pltpu.make_async_copy(early_ref.at[:, half:], right_ref.at[last, :], sems.at[1]),
    ]
    for copy in copies:
        copy.start()
    split_vector(v_ref, vv_ref)
    acc_ref[...] = jnp.zeros_like(acc_ref)

    def place(step, tile):
        rows = pl.ds(pl.multiple_of(step * tall, tall), tall)
        return rows, slice(tile * wide, (tile + 1) * wide)

    def squares(step, tile):
        rows, columns = place(step, tile)
        return jnp.dot(fj_ref[rows, :], fi_ref[:, columns], preferred_element_type=jnp.float32)

    ahead_ref[...] = squares(0, 0)

    @pl.loop(0, steps)
    def _(step):
        squared = ahead_ref[...]
        for tile in range(tiles):
            if tile + 1 < tiles:
                ahead = squares(step, tile + 1)
            else:
                ahead = squares(jnp.minimum(step + 1, steps - 1), 0)
            rows, columns = place(step, tile)
            value = value_of(squared)
            side, within = half_of((left_ref, right_ref), columns)
            side[rows, within] = value
            acc_ref[:, columns] += product(vv_ref[:, rows], value)
            squared = ahead
        ahead_ref[...] = squared

    for copy in copies:
        copy.wait()
    for c in range(out_ref.shape[0]):
        columns = slice(c * width, (c + 1) * width)
        side, within = half_of((left_ref, right_ref), columns)
        acc = acc_ref[:, columns] + product(vv_ref[:, last], side[last, within])
        out_ref[c] = FACTOR * (acc[:members] + acc[members:])


def build_and_product(v, fi, fj, early):
    members, width = v.shape[1:]
    rows, columns = fj.shape[0], fi.shape[1]
    return pl.pallas_call(
        build_body,
        out_shape=[
            pltpu.VMEM((rows, columns // 2), jnp.float32),
            pltpu.VMEM((rows, columns // 2), jnp.float32),
            jax.ShapeDtypeStruct((columns // width, members, width), jnp.float32),
        ],
        in_specs=[pl.BlockSpec(memory_space=VMEM)] * 3 + [pl.BlockSpec(memory_space=HBM)],
        out_specs=[pl.BlockSpec(memory_space=VMEM)] * 3,
        scratch_shapes=[
            pltpu.VMEM((2 * members, rows), jnp.bfloat16),
            pltpu.VMEM((2 * members, columns), jnp.float32),
            pltpu.VMEM((TALL, WIDE), jnp.float32),
            pltpu.SemaphoreType.DMA((2,)),
        ],
        compiler_params=pltpu.CompilerParams(vmem_limit_bytes=12 * MIB),
        cost_estimate=pl.CostEstimate(
            flops=40 * rows * columns, bytes_accessed=4 * rows * columns, transcendentals=0
        ),
        name="build",
    )(v, fi, fj, pltpu.with_memory_space_constraint(early, HBM))


def product_body(v_ref, left_ref, right_ref, out_ref, vv_ref):
    count, members, width = v_ref.shape
    split_vector(v_ref, vv_ref)
    for c in range(out_ref.shape[0]):
        columns = slice(c * width, (c + 1) * width)
        side, within = half_of((left_ref, right_ref), columns)
        acc = jnp.zeros((2 * members, width), jnp.float32)
        for r in range(count):
            rows = slice(r * width, (r + 1) * width)
            acc += product(vv_ref[:, rows], side[rows, within])
        out_ref[c] = FACTOR * (acc[:members] + acc[members:])


def kernel_product(v, left, right):
    _, members, width = v.shape
    rows, columns = left.shape[0], 2 * left.shape[1]
    return pl.pallas_call(
        product_body,
        out_shape=jax.ShapeDtypeStruct((columns // width, members, width), jnp.float32),
        in_specs=[pl.BlockSpec(memory_space=VMEM)] * 3,
        out_specs=pl.BlockSpec(memory_space=VMEM),
        scratch_shapes=[pltpu.VMEM((2 * members, rows), jnp.bfloat16)],
        compiler_params=pltpu.CompilerParams(vmem_limit_bytes=12 * MIB),
        cost_estimate=pl.CostEstimate(
            flops=128 * rows * columns, bytes_accessed=4 * rows * columns, transcendentals=0
        ),
        name="product",
    )(v, left, right)


def to_column(row, size):
    shape = (size, row.shape[1])
    same = lax.broadcasted_iota(jnp.int32, shape, 0) == lax.broadcasted_iota(jnp.int32, shape, 1)
    return jnp.sum(jnp.where(same, jnp.broadcast_to(row, shape), 0.0), axis=1, keepdims=True)


def terms_body(capacity, *refs):
    sources, (out_ref, z_ref, nugget_out_ref) = refs[:8], refs[8:11]
    t_ref, held_refs, sems = refs[11], refs[12:20], refs[20]
    chunk = sources[0].shape[0] // VALUE_COPIES
    parts = [slice(i * chunk, (i + 1) * chunk) for i in range(VALUE_COPIES)]
    pairs = [(sources[0].at[part], held_refs[0].at[part]) for part in parts]
    pairs = list(zip(sources[1:], held_refs[1:])) + pairs
    copies = [pltpu.make_async_copy(*pair, sems.at[i]) for i, pair in enumerate(pairs)]
    for copy in copies[1:7] + copies[:1] + copies[7:]:
        copy.start()
    values_ref, weights_ref, index_ref, count_ref, owner_ref, cov_ref, scale_ref, nugget_ref = held_refs
    slots, held = index_ref.shape
    members = values_ref.shape[0] // held
    lanes = slots * members
    group = 2 * slots

    for copy in copies[1:7]:
        copy.wait()
    z_ref[...] = cov_ref[...] / to_column(scale_ref[...], cov_ref.shape[0])
    nugget_out_ref[...] = nugget_ref[...]
    owner = owner_ref[...].astype(jnp.float32)
    square = (held, held)
    before = lax.broadcasted_iota(jnp.int32, square, 0) < lax.broadcasted_iota(jnp.int32, square, 1)
    shared = (to_column(owner, held) == owner) & before
    rank = jnp.sum(jnp.where(shared, 1.0, 0.0), axis=0, keepdims=True)
    devices = out_ref.shape[0]
    device = lax.broadcasted_iota(jnp.int32, (devices, held), 0).astype(jnp.float32)
    mine = jnp.where(device == owner, 1.0, 0.0)
    count = to_column(count_ref[...].astype(jnp.float32), held)
    index = index_ref[...].astype(jnp.float32)
    ranked = [jnp.where(rank == k, 1.0, 0.0) for k in range(capacity)]
    indices = [index * r for r in ranked]
    indices.append(jnp.zeros((lanes - capacity * slots, held), jnp.float32))
    out_ref[:, 0, capacity * lanes :] = lax.dot_general(
        mine.astype(jnp.bfloat16),
        jnp.concatenate(indices, axis=0).astype(jnp.bfloat16),
        (((1,), (1,)), ((), ())),
        preferred_element_type=jnp.float32,
    )

    copies[0].wait()
    lane = lax.broadcasted_iota(jnp.int32, (slots, lanes), 1)
    own = lane // members == lax.broadcasted_iota(jnp.int32, (slots, lanes), 0)
    for g in range(held // group):
        if g * group * members % chunk == 0:
            copies[7 + g * group * members // chunk].wait()
        weights = weights_ref[g * group * slots : (g + 1) * group * slots, :]
        values = values_ref[g * group * members : (g + 1) * group * members, :]
        every = lax.dot_general(
            weights, values, (((1,), (1,)), ((), ())), preferred_element_type=jnp.float32
        )
        rows = []
        for p in range(group):
            part = every[p * slots : (p + 1) * slots, p // slots * lanes : (p // slots + 1) * lanes]
            turn = (-(p % slots) * members) % lanes
            part = pltpu.roll(part, turn, 1) if turn else part
            part = pltpu.roll(part, 0, 1, stride=members, stride_axis=0)
            rows.append(jnp.sum(jnp.where(own, part, 0.0), axis=0, keepdims=True))
        t_ref[g * group : (g + 1) * group, :] = jnp.concatenate(rows, axis=0)
    slot = (lax.broadcasted_iota(jnp.int32, (held, lanes), 1) // members).astype(jnp.float32)
    terms = jnp.where(slot < count, t_ref[...], 0.0)
    payload = jnp.concatenate(thirds(terms), axis=1).astype(jnp.bfloat16)
    for k in range(capacity):
        table = (mine * ranked[k]).astype(jnp.bfloat16)
        placed = jnp.dot(table, payload, preferred_element_type=jnp.float32)
        out_ref[:, 0, k * lanes : (k + 1) * lanes] = (
            placed[:, :lanes] + placed[:, lanes : 2 * lanes]
        ) + placed[:, 2 * lanes :]


def terms_of(args, devices, capacity):
    values, _, index, _, _, covariates, _, nugget = args
    slots, held = index.shape
    lanes = slots * (values.shape[0] // held)
    return pl.pallas_call(
        functools.partial(terms_body, capacity),
        out_shape=[
            jax.ShapeDtypeStruct((devices, 1, (capacity + 1) * lanes), jnp.float32),
            jax.ShapeDtypeStruct(covariates.shape, jnp.float32),
            jax.ShapeDtypeStruct(nugget.shape, jnp.float32),
        ],
        in_specs=[pl.BlockSpec(memory_space=HBM)] * len(args),
        out_specs=[pl.BlockSpec(memory_space=VMEM)] * 3,
        scratch_shapes=[pltpu.VMEM((held, lanes), jnp.float32)]
        + [pltpu.VMEM(x.shape, x.dtype) for x in args]
        + [pltpu.SemaphoreType.DMA((len(args) - 1 + VALUE_COPIES,))],
        compiler_params=pltpu.CompilerParams(vmem_limit_bytes=8 * MIB),
        cost_estimate=pl.CostEstimate(flops=10**9, bytes_accessed=10**6, transcendentals=0),
        name="terms",
    )(*(pltpu.with_memory_space_constraint(x, HBM) for x in args))


def sources(axes, order):
    outer, inner = (lax.axis_index(name) for name in axes)
    sides = [lax.axis_size(name) for name in axes]
    for by_outer, by_inner in order:
        source = (outer - by_outer + sides[0]) % sides[0] * sides[1]
        yield source + (inner - by_inner + sides[1]) % sides[1]


def place_body(count, *refs):
    pieces, (fi_ref, fj_ref) = refs[:-2], refs[-2:]
    width = pieces[0].shape[2]
    blocks = [(ref, n) for ref in pieces[:count] for n in range(ref.shape[0])]
    sides = [lax.axis_size(name) for name in COL]
    order = [(at % sides[0], at // sides[0]) for at in range(len(blocks))]
    for (ref, n), source in zip(blocks, sources(COL, order)):
        columns = pl.ds(pl.multiple_of(source * width, width), width)
        fi_ref[:, columns] = features(ref[n] * SCALE, False).astype(jnp.bfloat16)
    blocks = [(ref, n) for ref in pieces[count:] for n in range(ref.shape[0])]
    sides = [lax.axis_size(name) for name in ROW]
    order = [(at // sides[1], at % sides[1]) for at in range(len(blocks))]
    for (ref, n), source in zip(blocks, sources(ROW, order)):
        rows = pl.ds(pl.multiple_of(source * width, width), width)
        block = features(ref[n] * SCALE, True)
        fj_ref[rows, :] = jnp.transpose(block.astype(jnp.bfloat16))


def place(row_pieces, column_pieces):
    width = row_pieces[0].shape[2]
    rows = sum(piece.shape[0] for piece in row_pieces) * width
    columns = sum(piece.shape[0] for piece in column_pieces) * width
    return pl.pallas_call(
        functools.partial(place_body, len(row_pieces)),
        out_shape=[
            jax.ShapeDtypeStruct((128, rows), jnp.bfloat16),
            jax.ShapeDtypeStruct((columns, 128), jnp.bfloat16),
        ],
        in_specs=[pl.BlockSpec(memory_space=VMEM)] * len(row_pieces + column_pieces),
        out_specs=[pl.BlockSpec(memory_space=VMEM)] * 2,
        compiler_params=pltpu.CompilerParams(vmem_limit_bytes=4 * MIB),
        cost_estimate=pl.CostEstimate(flops=10**9, bytes_accessed=10**6, transcendentals=0),
        name="place",
    )(*row_pieces, *column_pieces)


def gather_body(capacity, slots, message_ref, rhs_ref, copies_ref):
    devices = message_ref.shape[0]
    members, width = rhs_ref.shape
    lanes = slots * members
    index = jnp.transpose(message_ref[:, 0, capacity * lanes :])
    station = lax.broadcasted_iota(jnp.int32, (width, devices), 0).astype(jnp.float32)
    total = jnp.zeros((3 * members, width), jnp.float32)
    for k in range(capacity):
        terms = jnp.transpose(message_ref[:, 0, k * lanes : (k + 1) * lanes])
        split = [part.astype(jnp.bfloat16) for part in thirds(terms)]
        for s in range(slots):
            at = k * slots + s
            here = jnp.where(station == index[at : at + 1, :], 1.0, 0.0).astype(jnp.bfloat16)
            left = jnp.concatenate([p[s * members : (s + 1) * members] for p in split], axis=0)
            total += lax.dot_general(
                left, here, (((1,), (1,)), ((), ())), preferred_element_type=jnp.float32
            )
    rhs = total[:members] + (total[members : 2 * members] + total[2 * members :])
    rhs_ref[...] = rhs
    for r in range(copies_ref.shape[0]):
        copies_ref[r] = rhs


def gather_terms(message, shape, copies, capacity, slots):
    return pl.pallas_call(
        functools.partial(gather_body, capacity, slots),
        out_shape=[
            jax.ShapeDtypeStruct(shape, jnp.float32),
            jax.ShapeDtypeStruct((copies,) + shape, jnp.float32),
        ],
        in_specs=[pl.BlockSpec(memory_space=VMEM)],
        out_specs=[pl.BlockSpec(memory_space=VMEM)] * 2,
        compiler_params=pltpu.CompilerParams(vmem_limit_bytes=8 * MIB),
        cost_estimate=pl.CostEstimate(flops=10**9, bytes_accessed=10**6, transcendentals=0),
        name="gather",
    )(message)


def total_body(shares_ref, v_ref, nugget_ref, out_ref, copies_ref):
    total = nugget_ref[...] * v_ref[...]
    for c in range(shares_ref.shape[0]):
        total += shares_ref[c]
    out_ref[...] = total
    for r in range(copies_ref.shape[0]):
        copies_ref[r] = total


def total_of(shares, v, nugget, copies):
    return pl.pallas_call(
        total_body,
        out_shape=[
            jax.ShapeDtypeStruct(v.shape, jnp.float32),
            jax.ShapeDtypeStruct((copies,) + v.shape, jnp.float32),
        ],
        in_specs=[pl.BlockSpec(memory_space=VMEM)] * 3,
        out_specs=[pl.BlockSpec(memory_space=VMEM)] * 2,
        compiler_params=pltpu.CompilerParams(vmem_limit_bytes=4 * MIB),
        name="total",
    )(shares, v, nugget)


def guess_of(norm, energy):
    usable = energy > 0.5 * norm
    return jnp.where(usable, norm / jnp.where(usable, energy, 1.0), 0.0)


def close_body(shares_ref, rhs_ref, first_ref, nugget_ref, second_ref, sums_ref):
    rhs, first = rhs_ref[...], first_ref[...]
    second = nugget_ref[...] * first
    for c in range(shares_ref.shape[0]):
        second += shares_ref[c]
    second_ref[...] = second

    def dot(a, b):
        return jnp.sum(a * b, axis=1, keepdims=True)

    norm, energy = dot(rhs, rhs), dot(rhs, first)
    guess = guess_of(norm, energy)
    resid = rhs - guess * first
    along = first - guess * second
    sums = [
        norm,
        energy,
        dot(resid, resid),
        dot(resid, first),
        dot(first, first),
        dot(resid, along),
        dot(resid, second) + dot(first, along),
        dot(first, second),
    ]
    members = rhs.shape[0]
    shape = (members, len(sums) * members)
    row = lax.broadcasted_iota(jnp.int32, shape, 0)
    lane = lax.broadcasted_iota(jnp.int32, shape, 1)
    spaced = jnp.zeros(shape, jnp.float32)
    for at, column in enumerate(sums):
        here = lane == row + at * members
        spaced += jnp.where(here, jnp.broadcast_to(column, shape), 0.0)
    sums_ref[...] = jnp.broadcast_to(jnp.sum(spaced, axis=0, keepdims=True), sums_ref.shape)


def close(shares, rhs, first, nugget, devices):
    members = rhs.shape[0]
    return pl.pallas_call(
        close_body,
        out_shape=[
            jax.ShapeDtypeStruct(rhs.shape, jnp.float32),
            jax.ShapeDtypeStruct((devices, 8 * members), jnp.float32),
        ],
        in_specs=[pl.BlockSpec(memory_space=VMEM)] * 4,
        out_specs=[pl.BlockSpec(memory_space=VMEM)] * 2,
        compiler_params=pltpu.CompilerParams(vmem_limit_bytes=4 * MIB),
        name="close",
    )(shares, rhs, first, nugget)


def finish_body(
    sums_ref, rhs_ref, first_ref, second_ref, solved_out_ref, residual_out_ref, held_ref, sems
):
    rhs, first, second = rhs_ref[...], first_ref[...], second_ref[...]
    members = rhs.shape[0]
    norm, energy, rr, rf, ff, ra, rs, fs = (
        sums_ref[:, q * members : (q + 1) * members] for q in range(8)
    )

    def over(x):
        return jnp.sum(x, axis=0, keepdims=True)

    norm0 = over(norm)
    alpha0 = norm0 / over(energy)
    shift = alpha0 - guess_of(norm, energy)
    norm1 = over(rr - shift * (2.0 * rf - shift * ff))
    energy1 = over(ra - shift * (rs - shift * fs))
    ratio = norm1 / norm0
    alpha1 = norm1 / (energy1 - ratio * norm1 / alpha0)
    shape = (members, members)
    same = lax.broadcasted_iota(jnp.int32, shape, 0) == lax.broadcasted_iota(jnp.int32, shape, 1)

    def column(x):
        return jnp.sum(jnp.where(same, jnp.broadcast_to(x, shape), 0.0), axis=1, keepdims=True)

    alpha0, alpha1, ratio = column(alpha0), column(alpha1), column(ratio)
    residual = rhs - alpha0 * first
    direction = residual + ratio * rhs
    along = (first - alpha0 * second) + ratio * first
    held_ref[0] = alpha0 * rhs + alpha1 * direction
    held_ref[1] = residual - alpha1 * along
    copies = [
        pltpu.make_async_copy(held_ref.at[n], target, sems.at[n])
        for n, target in enumerate((solved_out_ref, residual_out_ref))
    ]
    for copy in copies:
        copy.start()
    for copy in copies:
        copy.wait()


def finish(sums, rhs, first, second):
    return pl.pallas_call(
        finish_body,
        out_shape=[jax.ShapeDtypeStruct(rhs.shape, jnp.float32)] * 2,
        in_specs=[pl.BlockSpec(memory_space=VMEM)] * 4,
        out_specs=[pl.BlockSpec(memory_space=HBM)] * 2,
        scratch_shapes=[
            pltpu.VMEM((2,) + rhs.shape, jnp.float32),
            pltpu.SemaphoreType.DMA((2,)),
        ],
        compiler_params=pltpu.CompilerParams(vmem_limit_bytes=4 * MIB),
        name="finish",
    )(sums, rhs, first, second)


def exchange(pieces, axes):
    return lax.all_to_all(pieces, axes, split_axis=0, concat_axis=0, tiled=True)


def local(
    covariates, lengthscale, nugget, patch_values, patch_weights, block_index, slot_count, owner
):
    devices = lax.axis_size(ALL)
    held, members, cells = patch_values.shape
    slots = patch_weights.shape[1]
    stations = nugget.shape[0]
    capacity = max(2, 2 * held // devices)

    message, z, nugget = terms_of(
        (
            patch_values.reshape(held * members, cells),
            patch_weights.reshape(held * slots, cells),
            block_index.T,
            slot_count[None, :],
            owner.T,
            covariates,
            lengthscale[None, :],
            nugget[None, :],
        ),
        devices,
        capacity,
    )
    own = z[None]
    row_near = [own] + ring(own, COL[0])
    row_joined = jnp.concatenate(row_near)
    column_near = [own] + ring(own, ROW[1])
    column_joined = jnp.concatenate(column_near)
    row_far = ring(row_joined, COL[1])
    column_far = ring(column_joined, ROW[0])
    fi, fj = place(row_near + row_far, column_near + column_far)
    early = build_early(fi, fj)
    message = exchange(message, ALL)
    rhs, copies = gather_terms(message, (members, stations), lax.axis_size(ROW), capacity, slots)
    gathered = exchange(copies, ROW)
    left, right, partial_value = build_and_product(gathered, fi, fj, early)
    shares = exchange(partial_value, COL)
    first, copies = total_of(shares, rhs, nugget, lax.axis_size(ROW))
    shares = exchange(kernel_product(exchange(copies, ROW), left, right), COL)
    second, sums = close(shares, rhs, first, nugget, devices)
    sums = exchange(sums[:, None, :], ALL)[:, 0, :]
    return finish(sums, rhs, first, second)


def solution(mesh):
    torus = Mesh(mesh.devices.reshape(4, 2, 4, 4), ALL)
    placed = (
        P(None, ALL),
        P(),
        P(ALL),
        P(ALL, None, None),
        P(ALL, None, None),
        P(ALL, None),
        P(ALL),
        P(ALL, None),
    )
    return jax.shard_map(
        local,
        mesh=torus,
        in_specs=placed,
        out_specs=(P(None, ALL), P(None, ALL)),
        check_vma=False,
    )
```
